256 devices in a mesh: fft: 32 (over z, y), band: 8 (over x, core).
Axes of the slice: x: 4, y: 4, z: 8, core: 2. Of those that a mesh axis runs over, the one named last changes fastest.
Arguments:
- coefficients: bfloat16 [96, 737280], P('band', 'fft'), may hold values from -0.0390625 to 0.0390625
- occupations: float32 [96], P('band'), may hold values from 0.5 to 2
- columns: int32 [5120], P('fft'), may hold values from 0 to 5183
- counts: int32 [32], P('fft'), may hold values from 1 to 160, 2048 in all
- plane_slot: int32 [160], replicated, may hold values from -1 to 143, as said below
Outputs:
- density: float32 [160, 144, 144], P('fft', 'band')
The draws below stay inside these ranges and needn't reach their ends.
Inputs may be any that keep to these rules, and one draw needn't show every extreme that they name: The counts sum to 2048, and one of them equals 160. `plane_slot`: every plane 0 .. 143 stands in exactly one slot; the other slots hold -1.
All inputs are finite; a program needn't handle non-finite values. No bound on the sum of `counts` on one device may be relied on, other than what follows from the above.
Results may differ from the reference program's by a relative error of at most 0.0095.
Values may be sent and summed in bfloat16 or wider, within the bound.
A program may use at most 192 MiB of HBM per device.

```python
import math
import jax
import jax.numpy as jnp
import numpy as np
from jax import lax

N = 144
GB = 72
STICK_DEV = 160
STICKS = 2048
STICKS_ALL = 5120
BANDS = 96
SLOTS = 160
N_FFT = 32


def draw_plane_slot(key, part):
    shuffled = jax.random.permutation(key, SLOTS)
    return jnp.where(shuffled < N, shuffled, -1).astype(jnp.int32)


def touch_ends(values, stream_key, least, high):
    longest = values.shape.index(max(values.shape))
    spots = []
    for shift in (0, 1):
        where = [jax.random.randint(jax.random.fold_in(stream_key, axis), (), 0, length) for axis, length in enumerate(values.shape)]
        where[longest] = (where[longest] + shift) % values.shape[longest]
        spots.append(tuple(where))
    return values.at[spots[0]].set(least).at[spots[1]].set(high)


def block_levels(rng, dims, cuts, least, top_value):
    def one(dim, parts):
        draws = jax.random.uniform(jax.random.fold_in(jax.random.fold_in(rng, 6), dim), (parts,), jnp.float32, least / len(cuts), top_value / len(cuts))
        return jnp.repeat(jnp.exp(draws), dims[dim] // parts).reshape((-1,) + (1,) * (len(dims) - dim - 1))

    loudness = one(*cuts[0])
    for cut in cuts[1:]:
        loudness = loudness * one(*cut)
    return loudness


def length_profile(count, total, limit, slope):
    loads = [(1 << 20) // math.isqrt(rank ** slope) + 1 for rank in range(2, count + 1)]
    surplus, given = total - limit - (count - 1), [1] * (count - 1)
    while surplus > 0:
        free = [i for i in range(count - 1) if given[i] < limit]
        mass, budget = sum([loads[i] for i in free]), surplus
        for i in free:
            extra = min(limit - given[i], max(1, budget * loads[i] // mass), surplus)
            given[i] = given[i] + extra
            surplus = surplus - extra
    return np.array([limit] + given)


def ragged_sizes(rng, count, total, reach, slope):
    if count == 2:
        one = jax.random.randint(rng, (), max(1, total - reach), min(reach, total - 1) + 1)
        return jnp.stack([one, total - one])
    lengths = jnp.asarray(length_profile(count, total, reach, slope), jnp.int32)
    twos = (count - 1) // 2
    donor, receiver = lengths[1:1 + 2 * twos:2], lengths[2:2 + 2 * twos:2]
    room = jnp.minimum(donor - 1, reach - receiver)
    shifted = jax.random.randint(jax.random.fold_in(rng, 1), (twos,), 0, 1 << 20) % (room + 1)
    lengths = lengths.at[1:1 + 2 * twos:2].set(donor - shifted).at[2:2 + 2 * twos:2].set(receiver + shifted)
    return lengths[jax.random.permutation(jax.random.fold_in(rng, 2), count)]


def scatter_about(stream_key, shape, width, limit, shards=(), kind=jnp.bfloat16):
    level = block_levels(stream_key, shape, shards, -0.22, 0.18) if shards else 1.0
    entries = jax.random.normal(stream_key, shape, jnp.float32) * width * level
    return jnp.minimum(jnp.maximum(entries, -limit), limit).astype(kind)


def setup_inputs(seed: int = 0) -> dict:
    streams_of = jax.random.split(jax.random.key(seed), 6)
    coefficients = scatter_about(streams_of[0], (BANDS, STICKS_ALL * 2 * GB), (1.0 / (STICKS * GB) ** 0.5), 0.0390625, ((0, 8), (1, 32)))
    occupations = jnp.clip(jnp.exp(math.log(2.0) - 1.3862944 * jax.random.uniform(streams_of[1], (BANDS,), jnp.float32) ** block_levels(streams_of[1], (BANDS,), ((0, 8),), -0.2, 0.2)), 0.5, 2.0)
    columns = touch_ends(jax.random.randint(streams_of[2], (STICKS_ALL,), 0, GB * GB), jax.random.fold_in(streams_of[2], 1), 0, (GB * GB) - 1).astype(jnp.int32)
    counts = ragged_sizes(streams_of[3], N_FFT, STICKS, STICK_DEV, 2).astype(jnp.int32)
    plane_slot = draw_plane_slot(jax.random.fold_in(streams_of[5], 71), 0)
    return {"coefficients": coefficients, "occupations": occupations, "columns": columns, "counts": counts, "plane_slot": plane_slot}


def phase_pair(freq_count, positions, grid):
    freqs = jnp.arange(freq_count, dtype=jnp.int32) - freq_count // 2
    turns = jnp.mod(freqs[:, None] * positions[None, :], grid)
    angles = turns.astype(jnp.float32) * (2.0 * math.pi / grid)
    return jnp.cos(angles), jnp.sin(angles)


def stick_table(plane_slot):
    valid_slot = (plane_slot >= 0).astype(jnp.float32)
    cosine, sine_part = phase_pair(GB, jnp.maximum(plane_slot, 0), N)
    cosine = cosine * valid_slot[None, :]
    sine_part = sine_part * valid_slot[None, :]
    upper_rows = jnp.concatenate([cosine, sine_part], axis=1)
    lower_rows = jnp.concatenate([-sine_part, cosine], axis=1)
    return jnp.concatenate([upper_rows, lower_rows], axis=0).astype(jnp.bfloat16)


def row_table():
    cosine, sine_part = phase_pair(GB, jnp.arange(N, dtype=jnp.int32), N)
    upper_rows = jnp.concatenate([cosine, sine_part], axis=1)
    lower_rows = jnp.concatenate([-sine_part, cosine], axis=1)
    return jnp.concatenate([upper_rows, lower_rows], axis=0).astype(jnp.bfloat16)


def column_table():
    cosine, sine_part = phase_pair(GB, jnp.arange(N, dtype=jnp.int32), N)
    return jnp.concatenate([cosine.T, sine_part.T], axis=0).astype(jnp.bfloat16)


def grid_squares(received, real_index, imag_index, row_tab, col_tab):
    bands_here, _, planes, _ = received.shape
    flat_plane = jnp.zeros((bands_here, planes, GB * 2 * GB), jnp.float32)
    flat_plane = flat_plane.at[:, :, real_index].add(received[:, 0].astype(jnp.float32))
    flat_plane = flat_plane.at[:, :, imag_index].add(received[:, 1].astype(jnp.float32))
    g_plane = flat_plane.reshape(bands_here, planes, GB, 2 * GB).astype(jnp.bfloat16)
    half_way = jnp.einsum("bpgk,kj->bpgj", g_plane.astype(jnp.float32), row_tab.astype(jnp.float32)).astype(jnp.bfloat16)
    full_grid = jnp.einsum("xg,bpgj->bpxj", col_tab.astype(jnp.float32), half_way.astype(jnp.float32))
    real_part = full_grid[:, :, :N, :N] - full_grid[:, :, N:, N:]
    imag_part = full_grid[:, :, N:, :N] + full_grid[:, :, :N, N:]
    return real_part * real_part + imag_part * imag_part


def reference(coefficients, occupations, columns, counts, plane_slot):
    shaped = coefficients.reshape(BANDS, STICKS_ALL, 2 * GB)
    stick_place = jnp.arange(STICKS_ALL, dtype=jnp.int32)
    live_stick = (stick_place % STICK_DEV < jnp.repeat(counts, STICK_DEV)).astype(jnp.bfloat16)
    masked = shaped * live_stick[None, :, None]
    real_index = (columns // GB) * (2 * GB) + columns % GB
    imag_index = real_index + GB
    plane_tab = stick_table(plane_slot)
    row_tab = row_table()
    col_tab = column_table()

    def one_band(running, inputs):
        coeffs, weight = inputs
        sticks = jnp.dot(coeffs, plane_tab, preferred_element_type=jnp.float32).astype(jnp.bfloat16)
        outgoing = sticks.T.reshape(1, 2, SLOTS, STICKS_ALL)
        squares = grid_squares(outgoing, real_index, imag_index, row_tab, col_tab)
        return running + weight * squares[0], None

    start = jnp.zeros((SLOTS, N, N), jnp.float32)
    density, _ = lax.scan(one_band, start, (masked, occupations / BANDS))
    return density
```

```python
import functools

import jax
import jax.numpy as jnp
import numpy as np
from jax import lax
from jax.experimental import pallas as pl
from jax.experimental.pallas import tpu as pltpu
from jax.sharding import PartitionSpec as P

N = 144
GB = 72
BANDS_HERE = 12
SLOTS = 160
PLANES = 5
NF = 32
NB = 8
Z, Y = 8, 4
PAIRS = 15
ROWS = 32
TILES = 40
KALL = TILES * 128
CHUNKS = 5
XB = N // NB
F32 = jnp.float32
BF16 = jnp.bfloat16
MESH = pl.DeviceIdType.MESH

NT = (((1,), (1,)), ((), ()))


def trig(freqs, positions):
    turns = np.mod(freqs[:, None] * positions[None, :], N)
    angles = turns * (2.0 * np.pi / N)
    return np.cos(angles), np.sin(angles)


def stick_rows():
    cosine, sine = trig(np.arange(GB) - GB // 2, np.arange(N))
    rows = np.zeros((2 * N, 256), np.float32)
    rows[:N, :GB] = cosine.T
    rows[:N, GB : 2 * GB] = -sine.T
    rows[N:, :GB] = sine.T
    rows[N:, GB : 2 * GB] = cosine.T
    return jnp.asarray(rows, BF16)


def row_table():
    cosine, sine = trig(np.arange(GB) - GB // 2, np.arange(N))
    table = np.zeros((2, 256, 6, 256), np.float32)
    for third in range(3):
        at = slice(third * GB, (third + 1) * GB)
        table[0, at, third * 2, :N] = cosine
        table[0, at, third * 2 + 1, :N] = sine
        table[1, at, third * 2, :N] = -sine
        table[1, at, third * 2 + 1, :N] = cosine
    return jnp.asarray(table.reshape(512, 1536), BF16)


def column_table():
    cosine, sine = trig(np.arange(GB) - GB // 2, np.arange(N))
    table = np.zeros((2, N, 6, 32), np.float32)
    for third in range(3):
        c, s = cosine[third::3].T, sine[third::3].T
        table[0, :, third * 2, :24] = c
        table[0, :, third * 2 + 1, :24] = -s
        table[1, :, third * 2, :24] = s
        table[1, :, third * 2 + 1, :24] = c
    return jnp.asarray(table.reshape(2 * N, 192), BF16)


SEND_ORDER = [4 * dz + dy for dz in (4, 3, 5, 2, 6, 1, 7, 0) for dy in (2, 1, 3, 0)]
SEND_ORDER = [o for o in SEND_ORDER if o]


def kernel(
    x_ref, psel_ref, cols_ref, counts_ref, occ_ref, trow_ref, rt_ref, ct_ref,
    out_ref,
    w_ref, xc_ref, send_ref, rec_ref, rem_ref, hm_ref, oht_ref, lhs_ref,
    g_ref, hs_ref, sum_ref, stage_ref, bsend_ref, brec_ref, tot_ref,
    ssem, rsem, bssem, brsem,
):
    me = lax.axis_index("fft")
    band = lax.axis_index("band")
    my_z, my_y = me // Y, lax.rem(me, Y)

    def peer(o):
        dz, dy = o // Y, o % Y
        return lax.rem(my_z + dz, Z) * Y + lax.rem(my_y + dy, Y)

    barrier = pltpu.get_barrier_semaphore()
    for o in range(1, NF):
        pl.semaphore_signal(barrier, inc=1, device_id=(peer(o), band), device_id_type=MESH)
    for o in range(1, NB):
        pl.semaphore_signal(
            barrier, inc=1, device_id=(me, lax.rem(band + o, NB)), device_id_type=MESH
        )

    chosen = lax.broadcasted_iota(jnp.int32, (NF * ROWS, 2 * N), 1) == psel_ref[...]
    base = jnp.dot(
        jnp.where(chosen, 1.0, 0.0).astype(BF16), trow_ref[...], preferred_element_type=F32
    )
    row = lax.broadcasted_iota(jnp.int32, (NF * ROWS, 256), 0)
    within = lax.rem(row, 16)
    for bg in range(3):
        keep = (within >= bg * 5) & (within < bg * 5 + 5)
        w_ref[:, bg * 256 : (bg + 1) * 256] = jnp.where(keep, base, 0.0).astype(BF16)

    xc_ref[...] = jnp.zeros_like(xc_ref)
    for bg in range(3):
        for b4 in range(4):
            first = (bg * 4 + b4) * SLOTS
            xc_ref[1 + b4, :, bg * 256 : bg * 256 + 144] = x_ref[first : first + 128, :]
            xc_ref[0, 32 * b4 : 32 * b4 + 32, bg * 256 : bg * 256 + 144] = x_ref[
                first + 128 : first + SLOTS, :
            ]

    lane = lax.broadcasted_iota(jnp.int32, (1, 128), 1)
    count = counts_ref[0]
    row32 = lax.broadcasted_iota(jnp.int32, (ROWS, 128), 0)

    def outgoing(c):
        is_rem = c == 0
        slot = jnp.where(is_rem, 128 + lax.rem(lane, 32), lane)
        live = jnp.where(slot < count, 1.0, 0.0)
        res = lax.dot_general(w_ref[...], xc_ref[c], NT, preferred_element_type=F32) * live
        col = cols_ref[pl.ds(jnp.minimum(c, 1), 1), :]
        gx = jnp.floor((col + 0.5) * (1.0 / GB))
        gy = col - gx * GB
        aux = jnp.where(row32 == 15, gx, jnp.where(row32 == 31, gy, 0.0))
        send_ref[c] = (res.reshape(NF, ROWS, 128) + aux[None]).astype(BF16)

    def block_copy(c, o):
        return pltpu.make_async_remote_copy(
            src_ref=send_ref.at[c, peer(o)],
            dst_ref=rec_ref.at[c, o],
            send_sem=ssem.at[c],
            recv_sem=rsem.at[c],
            device_id=(peer(o), band),
            device_id_type=MESH,
        )

    def all_blocks(c):
        return pltpu.make_async_remote_copy(
            src_ref=send_ref.at[c, pl.ds(1, NF - 1)],
            dst_ref=rec_ref.at[c, pl.ds(1, NF - 1)],
            send_sem=ssem.at[c],
            recv_sem=rsem.at[c],
            device_id=(peer(1), band),
            device_id_type=MESH,
        )

    outgoing(0)
    pl.semaphore_wait(barrier, NF - 1 + NB - 1)

    def send_chunk(c, carry):
        @pl.when(c > 0)
        def _():
            outgoing(c)

        for o in SEND_ORDER:
            block_copy(c, o).start()
        rec_ref[c, 0] = send_ref[c, me]
        return carry

    lax.fori_loop(0, CHUNKS, send_chunk, 0)

    sum_ref[...] = jnp.zeros_like(sum_ref)

    all_blocks(0).wait_recv()

    def shuffle(g, carry):
        tiles = [rec_ref[0, 4 * g + j].astype(F32) for j in range(4)]
        quarter = lax.broadcasted_iota(jnp.int32, (ROWS, 128), 1) // 32
        for b4 in range(4):
            done = jnp.zeros((ROWS, 128), F32)
            for j in range(4):
                shift = (32 * (j - b4)) % 128
                moved = tiles[j] if shift == 0 else pltpu.roll(tiles[j], shift, 1)
                done = jnp.where(quarter == j, moved, done)
            rem_ref[b4, g] = done.astype(BF16)
        return carry

    lax.fori_loop(0, 8, shuffle, 0)

    all_blocks(1).wait_recv()

    def picks(tile, o):
        at = pl.ds(pl.multiple_of(o * 128, 128), 128)
        values = tile.astype(F32)
        gx, gy = values[15:16], values[31:32]
        hi = jnp.floor((gx + 0.5) * (1.0 / 3.0))
        lo = (gx - 3.0 * hi) * GB + gy
        h = lax.broadcasted_iota(jnp.int32, (32, 128), 0).astype(F32)
        hm_ref[:, at] = jnp.where(h == hi, 1.0, 0.0).astype(BF16)
        k = lax.broadcasted_iota(jnp.int32, (256, 128), 0).astype(F32)
        oht_ref[:, at] = jnp.where(k == lo, 1.0, 0.0).astype(BF16)

    def main_picks(o, carry):
        picks(rec_ref[1, o], o)
        return carry

    def rem_picks(g, carry):
        picks(rem_ref[0, g], 32 + g)
        return carry

    lax.fori_loop(0, NF, main_picks, 0)
    lax.fori_loop(0, 8, rem_picks, 0)

    def spread(tile, o):
        at = pl.ds(pl.multiple_of(o * 128, 128), 128)
        values = tile.astype(F32)
        top, low = hm_ref[0:16, at], hm_ref[16:32, at]
        for part in range(2):
            for r in range(PAIRS):
                q = part * 16 + r
                line = jnp.broadcast_to(values[q : q + 1], (16, 128)).astype(BF16)
                m = (part * PAIRS + r) * 32
                lhs_ref[m : m + 16, at] = line * top
                lhs_ref[m + 16 : m + 32, at] = line * low

    def stage(b4, carry):
        @pl.when(b4 > 0)
        def _():
            all_blocks(1 + b4).wait_recv()

        def main_spread(o, c):
            spread(rec_ref[1 + b4, o], o)
            return c

        def rem_spread(g, c):
            spread(rem_ref[b4, g], 32 + g)
            return c

        lax.fori_loop(0, NF, main_spread, 0)
        lax.fori_loop(0, 8, rem_spread, 0)
        for part in range(2):
            placed = lax.dot_general(
                lhs_ref[part * 480 : (part + 1) * 480, :], oht_ref[...], NT,
                preferred_element_type=F32,
            )
            g_ref[:, part * 256 : (part + 1) * 256] = placed.astype(BF16)
        for block in range(6):
            half = jnp.dot(
                g_ref[...], rt_ref[:, block * 256 : (block + 1) * 256],
                preferred_element_type=F32,
            )
            hs_ref[:, block * 32 : (block + 1) * 32, :] = half.astype(BF16).reshape(
                PAIRS, 32, 256
            )
        for p in range(PLANES):
            total = sum_ref[p]
            for bg in range(3):
                wave = jnp.dot(ct_ref[...], hs_ref[bg * 5 + p], preferred_element_type=F32)
                re, im = wave[:N], wave[N:]
                total += (re * re + im * im) * occ_ref[bg * 4 + b4]
            sum_ref[p] = total
        return carry

    lax.fori_loop(0, 4, stage, 0)

    for j in range(NB):
        for p in range(PLANES):
            stage_ref[j, XB * p : XB * (p + 1), :] = sum_ref[p, XB * j : XB * (j + 1), :]
        stage_ref[j, 90:96, :] = jnp.zeros((6, 256), F32)
        bsend_ref[j] = stage_ref[j].astype(BF16)
    for o in range(1, NB):
        to = lax.rem(band + o, NB)
        pltpu.make_async_remote_copy(
            src_ref=bsend_ref.at[to],
            dst_ref=brec_ref.at[o],
            send_sem=bssem,
            recv_sem=brsem,
            device_id=(me, to),
            device_id_type=MESH,
        ).start()
    band_blocks = pltpu.make_async_remote_copy(
        src_ref=bsend_ref.at[pl.ds(1, NB - 1)],
        dst_ref=brec_ref.at[pl.ds(1, NB - 1)],
        send_sem=bssem,
        recv_sem=brsem,
        device_id=(me, lax.rem(band + 1, NB)),
        device_id_type=MESH,
    )
    total = stage_ref[band]
    band_blocks.wait_recv()
    for o in range(1, NB):
        total += brec_ref[o].astype(F32)
    tot_ref[...] = total
    for p in range(PLANES):
        out_ref[p] = tot_ref[XB * p : XB * (p + 1), :N]
    for c in range(CHUNKS):
        all_blocks(c).wait_send()
    band_blocks.wait_send()


def shards(coefficients, occupations, columns, counts, plane_slot):
    x = coefficients.reshape(BANDS_HERE * SLOTS, 2 * GB)
    slots = jnp.broadcast_to(plane_slot.reshape(NF, 1, 1, PLANES), (NF, 2, 3, PLANES))
    slots = jnp.where(slots >= 0, slots + jnp.array([0, N], jnp.int32)[None, :, None, None], -1)
    slots = jnp.pad(slots.reshape(NF, 2, PAIRS), ((0, 0), (0, 0), (0, 1)), constant_values=-1)
    psel = slots.reshape(NF * ROWS, 1)
    cols = columns.astype(F32)
    cols = jnp.stack([jnp.tile(cols[128:], 4), cols[:128]])
    weights = occupations / (BANDS_HERE * NB)
    vmem = pl.BlockSpec(memory_space=pltpu.VMEM)
    smem = pl.BlockSpec(memory_space=pltpu.SMEM)
    return pl.pallas_call(
        kernel,
        out_shape=jax.ShapeDtypeStruct((PLANES, XB, N), F32),
        in_specs=[vmem, vmem, vmem, smem, smem, vmem, vmem, vmem],
        out_specs=vmem,
        scratch_shapes=[
            pltpu.VMEM((NF * ROWS, 768), BF16),
            pltpu.VMEM((CHUNKS, 128, 768), BF16),
            pltpu.VMEM((CHUNKS, NF, ROWS, 128), BF16),
            pltpu.VMEM((CHUNKS, NF, ROWS, 128), BF16),
            pltpu.VMEM((4, 8, ROWS, 128), BF16),
            pltpu.VMEM((32, KALL), BF16),
            pltpu.VMEM((256, KALL), BF16),
            pltpu.VMEM((960, KALL), BF16),
            pltpu.VMEM((480, 512), BF16),
            pltpu.VMEM((PAIRS, 192, 256), BF16),
            pltpu.VMEM((PLANES, N, 256), F32),
            pltpu.VMEM((NB, 96, 256), F32),
            pltpu.VMEM((NB, 96, 256), BF16),
            pltpu.VMEM((NB, 96, 256), BF16),
            pltpu.VMEM((96, 256), F32),
            pltpu.SemaphoreType.DMA((CHUNKS,)),
            pltpu.SemaphoreType.DMA((CHUNKS,)),
            pltpu.SemaphoreType.DMA,
            pltpu.SemaphoreType.DMA,
        ],
        compiler_params=pltpu.CompilerParams(
            collective_id=0, has_side_effects=True, vmem_limit_bytes=60 * 1024 * 1024
        ),
    )(x, psel, cols, counts, weights, stick_rows(), row_table(), column_table())


def solution(mesh):
    placed = (P("band", "fft"), P("band"), P("fft"), P("fft"), P())
    return jax.shard_map(
        shards, mesh=mesh, in_specs=placed, out_specs=P("fft", "band", None), check_vma=False
    )
```

```python
import functools

import jax
import jax.numpy as jnp
import numpy as np
from jax import lax
from jax.experimental import pallas as pl
from jax.experimental.pallas import tpu as pltpu
from jax.sharding import PartitionSpec as P

N = 144
GB = 72
BANDS_HERE = 12
SLOTS = 160
PLANES = 5
NF = 32
NB = 8
Z, Y = 8, 4
PAIRS = 15
ROWS = 32
TILES = 40
KALL = TILES * 128
HI = 24
STEP = 4
STEPS = TILES // STEP
CHUNKS = 5
XB = N // NB
F32 = jnp.float32
BF16 = jnp.bfloat16
MESH = pl.DeviceIdType.MESH

NT = (((1,), (1,)), ((), ()))


def trig(freqs, positions):
    turns = np.mod(freqs[:, None] * positions[None, :], N)
    angles = turns * (2.0 * np.pi / N)
    return np.cos(angles), np.sin(angles)


def stick_rows():
    cosine, sine = trig(np.arange(GB) - GB // 2, np.arange(N))
    rows = np.zeros((2 * N, 256), np.float32)
    rows[:N, :GB] = cosine.T
    rows[:N, GB : 2 * GB] = -sine.T
    rows[N:, :GB] = sine.T
    rows[N:, GB : 2 * GB] = cosine.T
    return jnp.asarray(rows, BF16)


def row_table():
    cosine, sine = trig(np.arange(GB) - GB // 2, np.arange(N))
    table = np.zeros((2, 256, 6, 256), np.float32)
    for third in range(3):
        at = slice(third * GB, (third + 1) * GB)
        table[0, at, third * 2, :N] = cosine
        table[0, at, third * 2 + 1, :N] = sine
        table[1, at, third * 2, :N] = -sine
        table[1, at, third * 2 + 1, :N] = cosine
    return jnp.asarray(table.reshape(512, 1536), BF16)


def column_table():
    cosine, sine = trig(np.arange(GB) - GB // 2, np.arange(N))
    table = np.zeros((2, N, 6, HI), np.float32)
    for third in range(3):
        c, s = cosine[third::3].T, sine[third::3].T
        table[0, :, third * 2] = c
        table[0, :, third * 2 + 1] = -s
        table[1, :, third * 2] = s
        table[1, :, third * 2 + 1] = c
    return jnp.asarray(table.reshape(2 * N, 6 * HI), BF16)


FAR_ORDER = [4 * dz + dy for dz in (4, 3, 5, 2) for dy in (2, 1, 3, 0)]
NEAR_ORDER = [4 * dz + dy for dz in (6, 1, 7, 0) for dy in (2, 1, 3, 0)][:-1]


def iota(shape, dim):
    return lax.broadcasted_iota(jnp.int32, shape, dim)


def kernel(
    x_hbm, trow_hbm, rt_hbm, ct_hbm, cols_ref, slot_ref, counts_ref, occ_ref,
    out_ref,
    x_ref, trow_ref, rt_ref, ct_ref, xf_ref, xr_ref, chosen_ref, w_ref, xc_ref, aux_ref,
    send_ref, rec_ref, hm_ref, oh_ref, lhs_a, lhs_b, acc_ref,
    g_ref, hs_ref, sum_ref, stage_ref, bsend_ref, brec_ref, tot_ref,
    ldsem, ssem, rsem, bssem, brsem,
):
    me = lax.axis_index("fft")
    band = lax.axis_index("band")
    my_z, my_y = me // Y, lax.rem(me, Y)

    def peer(o):
        dz, dy = o // Y, o % Y
        return lax.rem(my_z + dz, Z) * Y + lax.rem(my_y + dy, Y)

    barrier = pltpu.get_barrier_semaphore()
    for o in range(1, NF):
        pl.semaphore_signal(barrier, inc=1, device_id=(peer(o), band), device_id_type=MESH)
    for o in range(1, NB):
        pl.semaphore_signal(
            barrier, inc=1, device_id=(me, lax.rem(band + o, NB)), device_id_type=MESH
        )

    loads = [
        pltpu.make_async_copy(src, dst, ldsem.at[i])
        for i, (src, dst) in enumerate(
            ((trow_hbm, trow_ref), (x_hbm, x_ref), (rt_hbm, rt_ref), (ct_hbm, ct_ref))
        )
    ]
    for load in loads:
        load.start()

    def choose(d, carry):
        shape = (ROWS, 2 * N)
        row = iota(shape, 0)
        within = lax.rem(row, 16)
        plane = jnp.where(within < PAIRS, lax.rem(within, PLANES), PLANES)
        index = jnp.full(shape, -1, jnp.int32)
        for p in range(PLANES):
            index = jnp.where(plane == p, slot_ref[d * PLANES + p], index)
        hit = (iota(shape, 1) - N * (row // 16) == index) & (index >= 0)
        chosen_ref[pl.ds(pl.multiple_of(d * ROWS, ROWS), ROWS), :] = jnp.where(
            hit, 1.0, 0.0
        ).astype(BF16)
        return carry

    lax.fori_loop(0, NF, choose, 0)
    loads[0].wait()
    base = jnp.dot(chosen_ref[...], trow_ref[...], preferred_element_type=F32)
    within = lax.rem(iota((NF * ROWS, 256), 0), 16)
    for bg in range(3):
        keep = (within >= bg * PLANES) & (within < bg * PLANES + PLANES)
        w_ref[:, bg * 256 : (bg + 1) * 256] = jnp.where(keep, base, 0.0).astype(BF16)

    shape = (SLOTS, 256)
    l = iota(shape, 1)
    r = lax.rem(l, 32)
    wanted = jnp.where(l < 128, 8 * lax.rem(l, 16) + l // 16, 128 + 8 * lax.rem(r, 4) + r // 4)
    order = jnp.where(iota(shape, 0) == wanted, 1.0, 0.0).astype(BF16)
    col = jnp.broadcast_to(cols_ref[...].astype(F32), (16, SLOTS))
    gx = jnp.floor((col + 0.5) * (1.0 / GB))
    gy = col - gx * GB
    natural = jnp.where(iota((16, SLOTS), 0) == 0, gx, gy).astype(BF16)
    ordered = jnp.dot(natural, order, preferred_element_type=F32)
    aux_ref[0] = ordered[0:8, 128:]
    aux_ref[1] = ordered[0:8, :128]

    loads[1].wait()

    def widen(g, carry):
        for t in range(9):
            at = pl.ds(pl.multiple_of(g * 1152 + t * 128, 128), 128)
            xf_ref[pl.ds(pl.multiple_of((g * 9 + t) * 16, 16), BANDS_HERE), :] = x_ref[
                :, at
            ].astype(F32)
        return carry

    lax.fori_loop(0, 20, widen, 0)
    lane20 = iota((20, 128), 1)
    for b in range(BANDS_HERE):
        bg, b4 = b // 4, b % 4
        tiles = [xf_ref[pl.ds(t * 16 + b, 20, 144), :] for t in range(9)]
        for t in range(8):
            if t == 0:
                first, second = tiles[0], tiles[1]
            else:
                second = pltpu.roll(tiles[t + 1], 128 - 16 * t, 1)
                first = jnp.where(
                    lane20 < 128 - 16 * t, pltpu.roll(tiles[t], 128 - 16 * t, 1), second
                )
            for e, value in enumerate((first, second)):
                lanes = slice(bg * 256 + e * 128, bg * 256 + e * 128 + 128)
                xc_ref[1 + b4, 16 * t : 16 * t + 16, lanes] = value[:16].astype(BF16)
                xr_ref[b4, 4 * t : 4 * t + 4, lanes] = value[16:20]
    for b4 in range(4):
        xc_ref[0, 32 * b4 : 32 * b4 + 32, :] = xr_ref[b4].astype(BF16)

    lane = iota((1, 128), 1)
    count = counts_ref[0]
    row32 = iota((ROWS, 128), 0)

    def outgoing(c):
        r = lax.rem(lane, 32)
        slot = jnp.where(
            c == 0, 128 + 8 * lax.rem(r, 4) + r // 4, 8 * lax.rem(lane, 16) + lane // 16
        )
        live = jnp.where(slot < count, 1.0, 0.0)
        res = lax.dot_general(w_ref[...], xc_ref[c], NT, preferred_element_type=F32) * live
        columns = aux_ref[jnp.minimum(c, 1)]
        aux = jnp.where(row32 == 15, columns[0:1], jnp.where(row32 == 31, columns[1:2], 0.0))
        send_ref[c] = (res.reshape(NF, ROWS, 128) + aux[None]).astype(BF16)

    def block_copy(c, o, half):
        return pltpu.make_async_remote_copy(
            src_ref=send_ref.at[c, peer(o)],
            dst_ref=rec_ref.at[c, o],
            send_sem=ssem.at[c],
            recv_sem=rsem.at[c, half],
            device_id=(peer(o), band),
            device_id_type=MESH,
        )

    def blocks(c, first, size, half):
        return pltpu.make_async_remote_copy(
            src_ref=send_ref.at[c, pl.ds(0, size)],
            dst_ref=rec_ref.at[c, pl.ds(first, size)],
            send_sem=ssem.at[c],
            recv_sem=rsem.at[c, half],
            device_id=(peer(1), band),
            device_id_type=MESH,
        )

    def wait_far(c):
        blocks(c, 8, 16, 0).wait_recv()

    def wait_near(c):
        blocks(c, 1, 15, 1).wait_recv()

    outgoing(0)
    pl.semaphore_wait(barrier, NF - 1 + NB - 1)

    def send_chunk(c, carry):
        @pl.when(c > 0)
        def _():
            outgoing(c)

        for o in FAR_ORDER:
            block_copy(c, o, 0).start()
        for o in NEAR_ORDER:
            block_copy(c, o, 1).start()
        rec_ref[c, 0] = send_ref[c, me]
        return carry

    lax.fori_loop(0, CHUNKS, send_chunk, 0)

    sum_ref[...] = jnp.zeros_like(sum_ref)

    wait_far(0)
    wait_near(0)

    def shuffle(g, carry):
        tiles = [rec_ref[0, 4 * g + j].astype(F32) for j in range(4)]
        quarter = iota((ROWS, 128), 1) // 32
        for b4 in range(4):
            done = jnp.zeros((ROWS, 128), F32)
            for j in range(4):
                shift = (32 * (j - b4)) % 128
                moved = tiles[j] if shift == 0 else pltpu.roll(tiles[j], shift, 1)
                done = jnp.where(quarter == j, moved, done)
            rec_ref[1 + b4, 32 + g] = done.astype(BF16)
        return carry

    lax.fori_loop(0, 8, shuffle, 0)

    wait_far(1)
    wait_near(1)

    def picks(o, carry):
        at = pl.ds(pl.multiple_of(o * 128, 128), 128)
        values = rec_ref[1, o].astype(F32)
        gx, gy = values[15:16], values[31:32]
        hi = jnp.floor((gx + 0.5) * (1.0 / 3.0))
        lo = (gx - 3.0 * hi) * GB + gy
        i = iota((48, 128), 0)
        h = jnp.where(i < 24, i, i - 24).astype(F32)
        hm_ref[:, at] = jnp.where(h == hi, 1.0, 0.0).astype(BF16)
        column = jnp.transpose(jnp.broadcast_to(lo, (8, 128)))[:, 0:1]
        k = iota((128, 256), 1).astype(F32)
        oh_ref[at, :] = jnp.where(k == column, 1.0, 0.0).astype(BF16)
        return carry

    lax.fori_loop(0, TILES, picks, 0)

    rows = [part * 16 + r for part in range(2) for r in range(PAIRS)]

    def first_tile(step):
        late = jnp.where(step < 8, 4 * step, 4 * step - 32)
        return jnp.where(step < 4, 8 + 4 * step, jnp.where(step < 6, 16 + 4 * step, late))

    def spread(b4, step, lhs_ref):
        for j in range(STEP):
            o = first_tile(step) + j
            at = pl.ds(pl.multiple_of(o * 128, 128), 128)
            values = rec_ref[1 + b4, o].astype(F32)
            picked = hm_ref[:, at]
            lanes = slice(j * 128, j * 128 + 128)
            for i in range(PAIRS):
                a = jnp.broadcast_to(values[rows[2 * i] : rows[2 * i] + 1], (8, 128))
                b = jnp.broadcast_to(values[rows[2 * i + 1] : rows[2 * i + 1] + 1], (8, 128))
                for e, pair in enumerate(((a, a), (a, b), (b, b))):
                    m = 48 * i + 16 * e
                    lhs_ref[m : m + 16, lanes] = (
                        jnp.concatenate(pair, axis=0).astype(BF16)
                        * picked[16 * e : 16 * e + 16]
                    )

    def place(step, lhs_ref, fresh):
        at = pl.ds(pl.multiple_of(first_tile(step) * 128, 128), STEP * 128)
        got = jnp.dot(lhs_ref[...], oh_ref[at, :], preferred_element_type=F32)
        acc_ref[...] = got if fresh else acc_ref[...] + got

    def stage(b4, carry):
        @pl.when(b4 > 0)
        def _():
            wait_far(1 + b4)

        spread(b4, 0, lhs_a)
        acc_ref[...] = jnp.zeros_like(acc_ref)

        def two(i, c):
            @pl.when((b4 > 0) & (i == 2))
            def _():
                wait_near(1 + b4)

            place(2 * i, lhs_a, False)
            spread(b4, 2 * i + 1, lhs_b)
            place(2 * i + 1, lhs_b, False)
            spread(b4, jnp.minimum(2 * i + 2, STEPS - 1), lhs_a)
            return c

        lax.fori_loop(0, STEPS // 2, two, 0)
        half_rows = PAIRS * HI
        g_ref[:, :256] = acc_ref[:half_rows].astype(BF16)
        g_ref[:, 256:] = acc_ref[half_rows:].astype(BF16)
        for block in range(6):
            half = jnp.dot(
                g_ref[...], rt_ref[:, block * 256 : (block + 1) * 256],
                preferred_element_type=F32,
            )
            hs_ref[:, block * HI : (block + 1) * HI, :] = half.reshape(PAIRS, HI, 256)
        for p in range(PLANES):
            total = sum_ref[p]
            for bg in range(3):
                wave = jnp.dot(
                    ct_ref[...], hs_ref[bg * PLANES + p].astype(BF16),
                    preferred_element_type=F32,
                )
                re, im = wave[:N], wave[N:]
                total += (re * re + im * im) * (occ_ref[bg * 4 + b4] * (1.0 / (BANDS_HERE * NB)))
            sum_ref[p] = total
        return carry

    loads[2].wait()
    loads[3].wait()
    lax.fori_loop(0, 4, stage, 0)

    folded = iota((16, 128), 1) // 16
    for j in range(NB):
        for p in range(PLANES):
            stage_ref[j, XB * p : XB * (p + 1), :] = sum_ref[p, XB * j : XB * (j + 1), :]
        stage_ref[j, 90:96, :] = jnp.zeros((6, 256), F32)
        extra = jnp.zeros((16, 128), F32)
        for i in range(6):
            piece = stage_ref[j, 16 * i : 16 * i + 16, 128:]
            if i:
                piece = pltpu.roll(piece, 16 * i, 1)
            extra = jnp.where(folded == i, piece, extra)
        bsend_ref[j, :96] = stage_ref[j, :, :128].astype(BF16)
        bsend_ref[j, 96:] = extra.astype(BF16)
    for o in range(1, NB):
        to = lax.rem(band + o, NB)
        pltpu.make_async_remote_copy(
            src_ref=bsend_ref.at[to],
            dst_ref=brec_ref.at[o],
            send_sem=bssem,
            recv_sem=brsem,
            device_id=(me, to),
            device_id_type=MESH,
        ).start()
    band_blocks = pltpu.make_async_remote_copy(
        src_ref=bsend_ref.at[pl.ds(1, NB - 1)],
        dst_ref=brec_ref.at[pl.ds(1, NB - 1)],
        send_sem=bssem,
        recv_sem=brsem,
        device_id=(me, lax.rem(band + 1, NB)),
        device_id_type=MESH,
    )
    total = bsend_ref[band].astype(F32)
    for c in range(CHUNKS):
        blocks(c, 0, NF - 1, 0).wait_send()
    band_blocks.wait_recv()
    for o in range(1, NB):
        total += brec_ref[o].astype(F32)
    tot_ref[:, :128] = total[:96]
    for i in range(6):
        piece = total[96:]
        if i:
            piece = pltpu.roll(piece, 128 - 16 * i, 1)
        tot_ref[16 * i : 16 * i + 16, 128:] = piece
    for p in range(PLANES):
        out_ref[p] = tot_ref[XB * p : XB * (p + 1), :N]
    band_blocks.wait_send()


def shards(coefficients, occupations, columns, counts, plane_slot):
    vmem = pl.BlockSpec(memory_space=pltpu.VMEM)
    smem = pl.BlockSpec(memory_space=pltpu.SMEM)
    hbm = pl.BlockSpec(memory_space=pl.ANY)
    rows = 2 * PAIRS * HI
    return pl.pallas_call(
        kernel,
        out_shape=jax.ShapeDtypeStruct((PLANES, XB, N), F32),
        in_specs=[hbm, hbm, hbm, hbm, vmem, smem, smem, smem],
        out_specs=vmem,
        scratch_shapes=[
            pltpu.VMEM((BANDS_HERE, SLOTS * 2 * GB), BF16),
            pltpu.VMEM((2 * N, 256), BF16),
            pltpu.VMEM((512, 1536), BF16),
            pltpu.VMEM((2 * N, 6 * HI), BF16),
            pltpu.VMEM((2880, 128), F32),
            pltpu.VMEM((4, 32, 768), F32),
            pltpu.VMEM((NF * ROWS, 2 * N), BF16),
            pltpu.VMEM((NF * ROWS, 768), BF16),
            pltpu.VMEM((CHUNKS, 128, 768), BF16),
            pltpu.VMEM((2, 8, 128), F32),
            pltpu.VMEM((CHUNKS, NF, ROWS, 128), BF16),
            pltpu.VMEM((CHUNKS, TILES, ROWS, 128), BF16),
            pltpu.VMEM((48, KALL), BF16),
            pltpu.VMEM((KALL, 256), BF16),
            pltpu.VMEM((rows, STEP * 128), BF16),
            pltpu.VMEM((rows, STEP * 128), BF16),
            pltpu.VMEM((rows, 256), F32),
            pltpu.VMEM((PAIRS * HI, 512), BF16),
            pltpu.VMEM((PAIRS, 6 * HI, 256), F32),
            pltpu.VMEM((PLANES, N, 256), F32),
            pltpu.VMEM((NB, 96, 256), F32),
            pltpu.VMEM((NB, 112, 128), BF16),
            pltpu.VMEM((NB, 112, 128), BF16),
            pltpu.VMEM((96, 256), F32),
            pltpu.SemaphoreType.DMA((4,)),
            pltpu.SemaphoreType.DMA((CHUNKS,)),
            pltpu.SemaphoreType.DMA((CHUNKS, 2)),
            pltpu.SemaphoreType.DMA,
            pltpu.SemaphoreType.DMA,
        ],
        compiler_params=pltpu.CompilerParams(
            collective_id=0, has_side_effects=True, vmem_limit_bytes=60 * 1024 * 1024
        ),
    )(
        coefficients, stick_rows(), row_table(), column_table(),
        columns.reshape(1, SLOTS), plane_slot, counts, occupations,
    )


def solution(mesh):
    placed = (P("band", "fft"), P("band"), P("fft"), P("fft"), P())
    return jax.shard_map(
        shards, mesh=mesh, in_specs=placed, out_specs=P("fft", "band", None), check_vma=False
    )
```

```python
import functools

import jax
import jax.numpy as jnp
import numpy as np
from jax import lax
from jax.experimental import pallas as pl
from jax.experimental.pallas import tpu as pltpu
from jax.sharding import PartitionSpec as P

N = 144
GB = 72
BANDS_HERE = 12
SLOTS = 160
PLANES = 5
NF = 32
NB = 8
Z, Y = 8, 4
PAIRS = 15
ROWS = 32
TILES = 40
KALL = TILES * 128
HI = 24
STEP = 4
STEPS = TILES // STEP
CHUNKS = 5
XB = N // NB
F32 = jnp.float32
BF16 = jnp.bfloat16
MESH = pl.DeviceIdType.MESH

NT = (((1,), (1,)), ((), ()))


def trig(freqs, positions):
    turns = np.mod(freqs[:, None] * positions[None, :], N)
    angles = turns * (2.0 * np.pi / N)
    return np.cos(angles), np.sin(angles)


def stick_rows():
    cosine, sine = trig(np.arange(GB) - GB // 2, np.arange(N))
    rows = np.zeros((2 * N, 256), np.float32)
    rows[:N, :GB] = cosine.T
    rows[:N, GB : 2 * GB] = -sine.T
    rows[N:, :GB] = sine.T
    rows[N:, GB : 2 * GB] = cosine.T
    return jnp.asarray(rows, BF16)


def row_table():
    cosine, sine = trig(np.arange(GB) - GB // 2, np.arange(N))
    table = np.zeros((2, 256, 6, 256), np.float32)
    for third in range(3):
        at = slice(third * GB, (third + 1) * GB)
        table[0, at, third * 2, :N] = cosine
        table[0, at, third * 2 + 1, :N] = sine
        table[1, at, third * 2, :N] = -sine
        table[1, at, third * 2 + 1, :N] = cosine
    return jnp.asarray(table.reshape(512, 1536), BF16)


def column_table():
    cosine, sine = trig(np.arange(GB) - GB // 2, np.arange(N))
    table = np.zeros((2, N, 6, HI), np.float32)
    for third in range(3):
        c, s = cosine[third::3].T, sine[third::3].T
        table[0, :, third * 2] = c
        table[0, :, third * 2 + 1] = -s
        table[1, :, third * 2] = s
        table[1, :, third * 2 + 1] = c
    return jnp.asarray(table.reshape(2 * N, 6 * HI), BF16)


FAR_ORDER = [4 * dz + dy for dz in (4, 3, 5, 2) for dy in (2, 1, 3, 0)]
NEAR_ORDER = [4 * dz + dy for dz in (6, 1, 7, 0) for dy in (2, 1, 3, 0)][:-1]


def iota(shape, dim):
    return lax.broadcasted_iota(jnp.int32, shape, dim)


def kernel(
    x_hbm, trow_hbm, rt_hbm, ct_hbm, cols_ref, slot_ref, counts_ref, occ_ref,
    out_ref,
    x_ref, trow_ref, rt_ref, ct_ref, xf_ref, xr_ref, chosen_ref, w_ref, xc_ref, code_ref, codes_ref,
    send_ref, rec_ref, hm_ref, oh_ref, lhs_a, lhs_b, acc_ref,
    g_ref, hs_ref, sum_ref, stage_ref, bsend_ref, brec_ref, tot_ref,
    ldsem, cssem, crsem, ssem, rsem, bssem, brsem,
):
    me = lax.axis_index("fft")
    band = lax.axis_index("band")
    my_z, my_y = me // Y, lax.rem(me, Y)

    def peer(o):
        dz, dy = o // Y, o % Y
        return lax.rem(my_z + dz, Z) * Y + lax.rem(my_y + dy, Y)

    barrier = pltpu.get_barrier_semaphore()
    for o in range(1, NF):
        pl.semaphore_signal(barrier, inc=1, device_id=(peer(o), band), device_id_type=MESH)
    for o in range(1, NB):
        pl.semaphore_signal(
            barrier, inc=1, device_id=(me, lax.rem(band + o, NB)), device_id_type=MESH
        )

    loads = [
        pltpu.make_async_copy(src, dst, ldsem.at[i])
        for i, (src, dst) in enumerate(
            ((trow_hbm, trow_ref), (x_hbm, x_ref), (rt_hbm, rt_ref), (ct_hbm, ct_ref))
        )
    ]
    for load in loads:
        load.start()

    def choose(d, carry):
        shape = (ROWS, 2 * N)
        row = iota(shape, 0)
        within = lax.rem(row, 16)
        plane = jnp.where(within < PAIRS, lax.rem(within, PLANES), PLANES)
        index = jnp.full(shape, -1, jnp.int32)
        for p in range(PLANES):
            index = jnp.where(plane == p, slot_ref[d * PLANES + p], index)
        hit = (iota(shape, 1) - N * (row // 16) == index) & (index >= 0)
        chosen_ref[pl.ds(pl.multiple_of(d * ROWS, ROWS), ROWS), :] = jnp.where(
            hit, 1.0, 0.0
        ).astype(BF16)
        return carry

    lax.fori_loop(0, NF, choose, 0)
    loads[0].wait()
    base = jnp.dot(chosen_ref[...], trow_ref[...], preferred_element_type=F32)
    within = lax.rem(iota((NF * ROWS, 256), 0), 16)
    for bg in range(3):
        keep = (within >= bg * PLANES) & (within < bg * PLANES + PLANES)
        w_ref[:, bg * 256 : (bg + 1) * 256] = jnp.where(keep, base, 0.0).astype(BF16)

    shape = (SLOTS, 256)
    l = iota(shape, 1)
    r = lax.rem(l, 32)
    wanted = jnp.where(l < 128, 8 * lax.rem(l, 16) + l // 16, 128 + 8 * lax.rem(r, 4) + r // 4)
    order = jnp.where(iota(shape, 0) == wanted, 1.0, 0.0).astype(BF16)
    col = jnp.broadcast_to(cols_ref[...].astype(F32), (16, SLOTS))
    gx = jnp.floor((col + 0.5) * (1.0 / GB))
    gy = col - gx * GB
    natural = jnp.where(iota((16, SLOTS), 0) == 0, gx, gy).astype(BF16)
    ordered = jnp.dot(natural, order, preferred_element_type=F32)
    code_ref[...] = ordered[0:1] * GB + ordered[1:2]

    loads[1].wait()

    def widen(g, carry):
        for t in range(9):
            at = pl.ds(pl.multiple_of(g * 1152 + t * 128, 128), 128)
            xf_ref[pl.ds(pl.multiple_of((g * 9 + t) * 16, 16), BANDS_HERE), :] = x_ref[
                :, at
            ].astype(F32)
        return carry

    lax.fori_loop(0, 20, widen, 0)
    lane20 = iota((20, 128), 1)
    for b in range(BANDS_HERE):
        bg, b4 = b // 4, b % 4
        tiles = [xf_ref[pl.ds(t * 16 + b, 20, 144), :] for t in range(9)]
        for t in range(8):
            if t == 0:
                first, second = tiles[0], tiles[1]
            else:
                second = pltpu.roll(tiles[t + 1], 128 - 16 * t, 1)
                first = jnp.where(
                    lane20 < 128 - 16 * t, pltpu.roll(tiles[t], 128 - 16 * t, 1), second
                )
            for e, value in enumerate((first, second)):
                lanes = slice(bg * 256 + e * 128, bg * 256 + e * 128 + 128)
                xc_ref[1 + b4, 16 * t : 16 * t + 16, lanes] = value[:16].astype(BF16)
                xr_ref[b4, 4 * t : 4 * t + 4, lanes] = value[16:20]
    for b4 in range(4):
        xc_ref[0, 32 * b4 : 32 * b4 + 32, :] = xr_ref[b4].astype(BF16)

    lane = iota((1, 128), 1)
    count = counts_ref[0]

    def outgoing(c):
        r = lax.rem(lane, 32)
        slot = jnp.where(
            c == 0, 128 + 8 * lax.rem(r, 4) + r // 4, 8 * lax.rem(lane, 16) + lane // 16
        )
        live = jnp.where(slot < count, 1.0, 0.0)
        res = lax.dot_general(w_ref[...], xc_ref[c], NT, preferred_element_type=F32) * live
        send_ref[c] = res.reshape(NF, ROWS, 128).astype(BF16)

    def block_copy(c, o, half):
        return pltpu.make_async_remote_copy(
            src_ref=send_ref.at[c, peer(o)],
            dst_ref=rec_ref.at[c, o],
            send_sem=ssem.at[c],
            recv_sem=rsem.at[c, half],
            device_id=(peer(o), band),
            device_id_type=MESH,
        )

    def blocks(c, first, size, half):
        return pltpu.make_async_remote_copy(
            src_ref=send_ref.at[c, pl.ds(0, size)],
            dst_ref=rec_ref.at[c, pl.ds(first, size)],
            send_sem=ssem.at[c],
            recv_sem=rsem.at[c, half],
            device_id=(peer(1), band),
            device_id_type=MESH,
        )

    def wait_far(c):
        blocks(c, 8, 16, 0).wait_recv()

    def wait_near(c):
        blocks(c, 1, 15, 1).wait_recv()

    def code_copy(o):
        return pltpu.make_async_remote_copy(
            src_ref=code_ref,
            dst_ref=codes_ref.at[o],
            send_sem=cssem,
            recv_sem=crsem,
            device_id=(peer(o), band),
            device_id_type=MESH,
        )

    outgoing(0)
    pl.semaphore_wait(barrier, NF - 1 + NB - 1)
    for o in FAR_ORDER + NEAR_ORDER:
        code_copy(o).start()
    codes_ref[0] = code_ref[...]

    def send_chunk(c, carry):
        @pl.when(c > 0)
        def _():
            outgoing(c)

        for o in FAR_ORDER:
            block_copy(c, o, 0).start()
        for o in NEAR_ORDER:
            block_copy(c, o, 1).start()
        rec_ref[c, 0] = send_ref[c, me]
        return carry

    lax.fori_loop(0, CHUNKS, send_chunk, 0)

    sum_ref[...] = jnp.zeros_like(sum_ref)

    every_code = pltpu.make_async_remote_copy(
        src_ref=codes_ref.at[pl.ds(1, NF - 1)],
        dst_ref=codes_ref.at[pl.ds(1, NF - 1)],
        send_sem=cssem,
        recv_sem=crsem,
        device_id=(peer(1), band),
        device_id_type=MESH,
    )
    every_code.wait_recv()

    def picks(o, code):
        at = pl.ds(pl.multiple_of(o * 128, 128), 128)
        hi = jnp.floor((code + 0.5) * (1.0 / (3 * GB)))
        lo = code - 3 * GB * hi
        i = iota((48, 128), 0)
        h = jnp.where(i < 24, i, i - 24).astype(F32)
        hm_ref[:, at] = jnp.where(h == hi, 1.0, 0.0).astype(BF16)
        k = iota((256, 128), 0).astype(F32)
        oh_ref[:, at] = jnp.where(k == lo, 1.0, 0.0).astype(BF16)

    def main_picks(o, carry):
        picks(o, codes_ref[o, :, :128])
        return carry

    def rem_picks(g, carry):
        quarter = iota((1, 128), 1) // 32
        code = codes_ref[4 * g, :, 128:]
        for j in range(1, 4):
            code = jnp.where(quarter == j, codes_ref[4 * g + j, :, 128:], code)
        picks(32 + g, code)
        return carry

    lax.fori_loop(0, NF, main_picks, 0)
    lax.fori_loop(0, 8, rem_picks, 0)

    wait_far(0)
    wait_near(0)

    def shuffle(g, carry):
        tiles = [rec_ref[0, 4 * g + j].astype(F32) for j in range(4)]
        quarter = iota((ROWS, 128), 1) // 32
        for b4 in range(4):
            done = jnp.zeros((ROWS, 128), F32)
            for j in range(4):
                shift = (32 * (j - b4)) % 128
                moved = tiles[j] if shift == 0 else pltpu.roll(tiles[j], shift, 1)
                done = jnp.where(quarter == j, moved, done)
            rec_ref[1 + b4, 32 + g] = done.astype(BF16)
        return carry

    lax.fori_loop(0, 8, shuffle, 0)

    rows = [part * 16 + r for part in range(2) for r in range(PAIRS)]

    def first_tile(step):
        late = jnp.where(step < 8, 4 * step, 4 * step - 32)
        return jnp.where(step < 4, 8 + 4 * step, jnp.where(step < 6, 16 + 4 * step, late))

    def spread(b4, step, lhs_ref):
        for j in range(STEP):
            o = first_tile(step) + j
            at = pl.ds(pl.multiple_of(o * 128, 128), 128)
            values = rec_ref[1 + b4, o].astype(F32)
            picked = hm_ref[:, at]
            lanes = slice(j * 128, j * 128 + 128)
            for i in range(PAIRS):
                a = jnp.broadcast_to(values[rows[2 * i] : rows[2 * i] + 1], (8, 128))
                b = jnp.broadcast_to(values[rows[2 * i + 1] : rows[2 * i + 1] + 1], (8, 128))
                for e, pair in enumerate(((a, a), (a, b), (b, b))):
                    m = 48 * i + 16 * e
                    lhs_ref[m : m + 16, lanes] = (
                        jnp.concatenate(pair, axis=0).astype(BF16)
                        * picked[16 * e : 16 * e + 16]
                    )

    def place(step, lhs_ref, fresh):
        at = pl.ds(pl.multiple_of(first_tile(step) * 128, 128), STEP * 128)
        got = lax.dot_general(lhs_ref[...], oh_ref[:, at], NT, preferred_element_type=F32)
        acc_ref[...] = got if fresh else acc_ref[...] + got

    def stage(b4, carry):
        wait_far(1 + b4)
        spread(b4, 0, lhs_a)
        acc_ref[...] = jnp.zeros_like(acc_ref)

        def two(i, c):
            @pl.when(i == 2)
            def _():
                wait_near(1 + b4)

            place(2 * i, lhs_a, False)
            spread(b4, 2 * i + 1, lhs_b)
            place(2 * i + 1, lhs_b, False)
            spread(b4, jnp.minimum(2 * i + 2, STEPS - 1), lhs_a)
            return c

        lax.fori_loop(0, STEPS // 2, two, 0)
        half_rows = PAIRS * HI
        g_ref[:, :256] = acc_ref[:half_rows].astype(BF16)
        g_ref[:, 256:] = acc_ref[half_rows:].astype(BF16)
        for block in range(6):
            half = jnp.dot(
                g_ref[...], rt_ref[:, block * 256 : (block + 1) * 256],
                preferred_element_type=F32,
            )
            hs_ref[:, block * HI : (block + 1) * HI, :] = half.reshape(PAIRS, HI, 256)
        for p in range(PLANES):
            total = sum_ref[p]
            for bg in range(3):
                wave = jnp.dot(
                    ct_ref[...], hs_ref[bg * PLANES + p].astype(BF16),
                    preferred_element_type=F32,
                )
                re, im = wave[:N], wave[N:]
                total += (re * re + im * im) * (occ_ref[bg * 4 + b4] * (1.0 / (BANDS_HERE * NB)))
            sum_ref[p] = total
        return carry

    loads[2].wait()
    loads[3].wait()
    lax.fori_loop(0, 4, stage, 0)

    folded = iota((16, 128), 1) // 16
    for j in range(NB):
        for p in range(PLANES):
            stage_ref[j, XB * p : XB * (p + 1), :] = sum_ref[p, XB * j : XB * (j + 1), :]
        stage_ref[j, 90:96, :] = jnp.zeros((6, 256), F32)
        extra = jnp.zeros((16, 128), F32)
        for i in range(6):
            piece = stage_ref[j, 16 * i : 16 * i + 16, 128:]
            if i:
                piece = pltpu.roll(piece, 16 * i, 1)
            extra = jnp.where(folded == i, piece, extra)
        bsend_ref[j, :96] = stage_ref[j, :, :128].astype(BF16)
        bsend_ref[j, 96:] = extra.astype(BF16)
    for o in range(1, NB):
        to = lax.rem(band + o, NB)
        pltpu.make_async_remote_copy(
            src_ref=bsend_ref.at[to],
            dst_ref=brec_ref.at[o],
            send_sem=bssem,
            recv_sem=brsem,
            device_id=(me, to),
            device_id_type=MESH,
        ).start()
    band_blocks = pltpu.make_async_remote_copy(
        src_ref=bsend_ref.at[pl.ds(1, NB - 1)],
        dst_ref=brec_ref.at[pl.ds(1, NB - 1)],
        send_sem=bssem,
        recv_sem=brsem,
        device_id=(me, lax.rem(band + 1, NB)),
        device_id_type=MESH,
    )
    total = bsend_ref[band].astype(F32)
    for c in range(CHUNKS):
        blocks(c, 0, NF - 1, 0).wait_send()
    band_blocks.wait_recv()
    for o in range(1, NB):
        total += brec_ref[o].astype(F32)
    tot_ref[:, :128] = total[:96]
    for i in range(6):
        piece = total[96:]
        if i:
            piece = pltpu.roll(piece, 128 - 16 * i, 1)
        tot_ref[16 * i : 16 * i + 16, 128:] = piece
    for p in range(PLANES):
        out_ref[p] = tot_ref[XB * p : XB * (p + 1), :N]
    band_blocks.wait_send()
    every_code.wait_send()


def shards(coefficients, occupations, columns, counts, plane_slot):
    vmem = pl.BlockSpec(memory_space=pltpu.VMEM)
    smem = pl.BlockSpec(memory_space=pltpu.SMEM)
    hbm = pl.BlockSpec(memory_space=pltpu.HBM)
    rows = 2 * PAIRS * HI
    return pl.pallas_call(
        kernel,
        out_shape=jax.ShapeDtypeStruct((PLANES, XB, N), F32),
        in_specs=[hbm, hbm, hbm, hbm, vmem, smem, smem, smem],
        out_specs=vmem,
        scratch_shapes=[
            pltpu.VMEM((BANDS_HERE, SLOTS * 2 * GB), BF16),
            pltpu.VMEM((2 * N, 256), BF16),
            pltpu.VMEM((512, 1536), BF16),
            pltpu.VMEM((2 * N, 6 * HI), BF16),
            pltpu.VMEM((2880, 128), F32),
            pltpu.VMEM((4, 32, 768), F32),
            pltpu.VMEM((NF * ROWS, 2 * N), BF16),
            pltpu.VMEM((NF * ROWS, 768), BF16),
            pltpu.VMEM((CHUNKS, 128, 768), BF16),
            pltpu.VMEM((1, 256), F32),
            pltpu.VMEM((NF, 1, 256), F32),
            pltpu.VMEM((CHUNKS, NF, ROWS, 128), BF16),
            pltpu.VMEM((CHUNKS, TILES, ROWS, 128), BF16),
            pltpu.VMEM((48, KALL), BF16),
            pltpu.VMEM((256, KALL), BF16),
            pltpu.VMEM((rows, STEP * 128), BF16),
            pltpu.VMEM((rows, STEP * 128), BF16),
            pltpu.VMEM((rows, 256), F32),
            pltpu.VMEM((PAIRS * HI, 512), BF16),
            pltpu.VMEM((PAIRS, 6 * HI, 256), F32),
            pltpu.VMEM((PLANES, N, 256), F32),
            pltpu.VMEM((NB, 96, 256), F32),
            pltpu.VMEM((NB, 112, 128), BF16),
            pltpu.VMEM((NB, 112, 128), BF16),
            pltpu.VMEM((96, 256), F32),
            pltpu.SemaphoreType.DMA((4,)),
            pltpu.SemaphoreType.DMA,
            pltpu.SemaphoreType.DMA,
            pltpu.SemaphoreType.DMA((CHUNKS,)),
            pltpu.SemaphoreType.DMA((CHUNKS, 2)),
            pltpu.SemaphoreType.DMA,
            pltpu.SemaphoreType.DMA,
        ],
        compiler_params=pltpu.CompilerParams(
            collective_id=0, has_side_effects=True, vmem_limit_bytes=60 * 1024 * 1024
        ),
    )(
        coefficients, stick_rows(), row_table(), column_table(),
        columns.reshape(1, SLOTS), plane_slot, counts, occupations,
    )


def solution(mesh):
    placed = (P("band", "fft"), P("band"), P("fft"), P("fft"), P())
    return jax.shard_map(
        shards, mesh=mesh, in_specs=placed, out_specs=P("fft", "band", None), check_vma=False
    )
```

```python
import functools

import jax
import jax.numpy as jnp
import numpy as np
from jax import lax
from jax.experimental import pallas as pl
from jax.experimental.pallas import tpu as pltpu
from jax.sharding import PartitionSpec as P

N = 144
GB = 72
BANDS_HERE = 12
SLOTS = 160
PLANES = 5
NF = 32
NB = 8
Z, Y = 8, 4
PAIRS = 15
ROWS = 32
TILES = 40
KALL = TILES * 128
HI = 24
STEP = 10
CHUNKS = 5
XB = N // NB
F32 = jnp.float32
BF16 = jnp.bfloat16
MESH = pl.DeviceIdType.MESH

NT = (((1,), (1,)), ((), ()))


def trig(freqs, positions):
    turns = np.mod(freqs[:, None] * positions[None, :], N)
    angles = turns * (2.0 * np.pi / N)
    return np.cos(angles), np.sin(angles)


def stick_rows():
    cosine, sine = trig(np.arange(GB) - GB // 2, np.arange(N))
    rows = np.zeros((2 * N, 256), np.float32)
    rows[:N, :GB] = cosine.T
    rows[:N, GB : 2 * GB] = -sine.T
    rows[N:, :GB] = sine.T
    rows[N:, GB : 2 * GB] = cosine.T
    return jnp.asarray(rows, BF16)


def row_table():
    cosine, sine = trig(np.arange(GB) - GB // 2, np.arange(N))
    table = np.zeros((2, 256, 6, 256), np.float32)
    for third in range(3):
        at = slice(third * GB, (third + 1) * GB)
        table[0, at, third * 2, :N] = cosine
        table[0, at, third * 2 + 1, :N] = sine
        table[1, at, third * 2, :N] = -sine
        table[1, at, third * 2 + 1, :N] = cosine
    return jnp.asarray(table.reshape(512, 1536), BF16)


def column_table():
    cosine, sine = trig(np.arange(GB) - GB // 2, np.arange(N))
    table = np.zeros((2, N, 6, HI), np.float32)
    for third in range(3):
        c, s = cosine[third::3].T, sine[third::3].T
        table[0, :, third * 2] = c
        table[0, :, third * 2 + 1] = -s
        table[1, :, third * 2] = s
        table[1, :, third * 2 + 1] = c
    return jnp.asarray(table.reshape(2 * N, 6 * HI), BF16)


ORDER = [Y * dz + dy for dz in (0, 4, 3, 5, 2, 6, 1, 7) for dy in range(Y)]


def iota(shape, dim):
    return lax.broadcasted_iota(jnp.int32, shape, dim)


def kernel(
    x_hbm, trow_hbm, rt_hbm, ct_hbm, cols_ref, slot_ref, counts_ref, occ_ref,
    out_ref,
    x_ref, trow_ref, rt_ref, ct_ref, xf_ref, xr_ref, chosen_ref, w_ref, xc_ref, code_ref, codes_ref,
    send_ref, rec_ref, hm_ref, oh_ref, lhs_a, lhs_b, acc_ref,
    g_ref, hs_ref, sum_ref, stage_ref, bsend_ref, brec_ref, tot_ref,
    ldsem, cssem, crsem, ssem, rsem, bssem, brsem,
):
    me = lax.axis_index("fft")
    band = lax.axis_index("band")
    my_z, my_y = me // Y, lax.rem(me, Y)

    def peer(o):
        dz, dy = o // Y, o % Y
        return lax.rem(my_z + dz, Z) * Y + lax.rem(my_y + dy, Y)

    barrier = pltpu.get_barrier_semaphore()
    for o in range(1, NF):
        pl.semaphore_signal(barrier, inc=1, device_id=(peer(o), band), device_id_type=MESH)
    for o in range(1, NB):
        pl.semaphore_signal(
            barrier, inc=1, device_id=(me, lax.rem(band + o, NB)), device_id_type=MESH
        )

    loads = [
        pltpu.make_async_copy(src, dst, ldsem.at[i])
        for i, (src, dst) in enumerate(
            ((trow_hbm, trow_ref), (x_hbm, x_ref), (rt_hbm, rt_ref), (ct_hbm, ct_ref))
        )
    ]
    for load in loads:
        load.start()

    def choose(d, carry):
        shape = (ROWS, 2 * N)
        row = iota(shape, 0)
        within = lax.rem(row, 16)
        plane = jnp.where(within < PAIRS, lax.rem(within, PLANES), PLANES)
        index = jnp.full(shape, -1, jnp.int32)
        for p in range(PLANES):
            index = jnp.where(plane == p, slot_ref[d * PLANES + p], index)
        hit = (iota(shape, 1) - N * (row // 16) == index) & (index >= 0)
        chosen_ref[pl.ds(pl.multiple_of(d * ROWS, ROWS), ROWS), :] = jnp.where(
            hit, 1.0, 0.0
        ).astype(BF16)
        return carry

    lax.fori_loop(0, NF, choose, 0)
    loads[0].wait()
    base = jnp.dot(chosen_ref[...], trow_ref[...], preferred_element_type=F32)
    within = lax.rem(iota((NF * ROWS, 256), 0), 16)
    for bg in range(3):
        keep = (within >= bg * PLANES) & (within < bg * PLANES + PLANES)
        w_ref[:, bg * 256 : (bg + 1) * 256] = jnp.where(keep, base, 0.0).astype(BF16)

    shape = (SLOTS, 256)
    l = iota(shape, 1)
    r = lax.rem(l, 32)
    wanted = jnp.where(l < 128, 8 * lax.rem(l, 16) + l // 16, 128 + 8 * lax.rem(r, 4) + r // 4)
    order = jnp.where(iota(shape, 0) == wanted, 1.0, 0.0).astype(BF16)
    col = jnp.broadcast_to(cols_ref[...].astype(F32), (16, SLOTS))
    gx = jnp.floor((col + 0.5) * (1.0 / GB))
    gy = col - gx * GB
    natural = jnp.where(iota((16, SLOTS), 0) == 0, gx, gy).astype(BF16)
    ordered = jnp.dot(natural, order, preferred_element_type=F32)
    code_ref[...] = ordered[0:1] * GB + ordered[1:2]

    loads[1].wait()

    def widen(g, carry):
        for t in range(9):
            at = pl.ds(pl.multiple_of(g * 1152 + t * 128, 128), 128)
            xf_ref[pl.ds(pl.multiple_of((g * 9 + t) * 16, 16), BANDS_HERE), :] = x_ref[
                :, at
            ].astype(F32)
        return carry

    lax.fori_loop(0, 20, widen, 0)
    lane20 = iota((20, 128), 1)
    for b in range(BANDS_HERE):
        bg, b4 = b // 4, b % 4
        tiles = [xf_ref[pl.ds(t * 16 + b, 20, 144), :] for t in range(9)]
        for t in range(8):
            if t == 0:
                first, second = tiles[0], tiles[1]
            else:
                second = pltpu.roll(tiles[t + 1], 128 - 16 * t, 1)
                first = jnp.where(
                    lane20 < 128 - 16 * t, pltpu.roll(tiles[t], 128 - 16 * t, 1), second
                )
            for e, value in enumerate((first, second)):
                lanes = slice(bg * 256 + e * 128, bg * 256 + e * 128 + 128)
                xc_ref[1 + b4, 16 * t : 16 * t + 16, lanes] = value[:16].astype(BF16)
                xr_ref[b4, 4 * t : 4 * t + 4, lanes] = value[16:20]
    for b4 in range(4):
        xc_ref[0, 32 * b4 : 32 * b4 + 32, :] = xr_ref[b4].astype(BF16)

    lane = iota((1, 128), 1)
    count = counts_ref[0]

    def outgoing(c):
        r = lax.rem(lane, 32)
        slot = jnp.where(
            c == 0, 128 + 8 * lax.rem(r, 4) + r // 4, 8 * lax.rem(lane, 16) + lane // 16
        )
        live = jnp.where(slot < count, 1.0, 0.0)
        res = lax.dot_general(w_ref[...], xc_ref[c], NT, preferred_element_type=F32) * live
        send_ref[c] = res.reshape(NF, ROWS, 128).astype(BF16)

    def block_copy(c, i):
        return pltpu.make_async_remote_copy(
            src_ref=send_ref.at[c, peer(ORDER[i])],
            dst_ref=rec_ref.at[c, i],
            send_sem=ssem.at[c],
            recv_sem=rsem.at[c, i // 16 if i != 16 else 2],
            device_id=(peer(ORDER[i]), band),
            device_id_type=MESH,
        )

    def blocks(c, first, size, group):
        return pltpu.make_async_remote_copy(
            src_ref=send_ref.at[c, pl.ds(0, size)],
            dst_ref=rec_ref.at[c, pl.ds(first, size)],
            send_sem=ssem.at[c],
            recv_sem=rsem.at[c, group],
            device_id=(peer(1), band),
            device_id_type=MESH,
        )

    def wait_one(c):
        blocks(c, 16, 1, 2).wait_recv()

    def wait_group(c, group):
        blocks(c, 1 + 16 * group, 15, group).wait_recv()

    def code_copy(i):
        return pltpu.make_async_remote_copy(
            src_ref=code_ref,
            dst_ref=codes_ref.at[i],
            send_sem=cssem,
            recv_sem=crsem,
            device_id=(peer(ORDER[i]), band),
            device_id_type=MESH,
        )

    outgoing(0)
    pl.semaphore_wait(barrier, NF - 1 + NB - 1)
    for i in range(1, NF):
        code_copy(i).start()
    codes_ref[0] = code_ref[...]

    def send_chunk(c, carry):
        @pl.when(c > 0)
        def _():
            outgoing(c)

        for i in range(1, NF):
            block_copy(c, i).start()
        rec_ref[c, 0] = send_ref[c, me]
        return carry

    lax.fori_loop(0, CHUNKS, send_chunk, 0)

    sum_ref[...] = jnp.zeros_like(sum_ref)

    every_code = pltpu.make_async_remote_copy(
        src_ref=codes_ref.at[pl.ds(1, NF - 1)],
        dst_ref=codes_ref.at[pl.ds(1, NF - 1)],
        send_sem=cssem,
        recv_sem=crsem,
        device_id=(peer(1), band),
        device_id_type=MESH,
    )
    every_code.wait_recv()

    identity = jnp.where(iota((128, 128), 0) == iota((128, 128), 1), 1.0, 0.0).astype(BF16)

    def picks(o, code):
        at = pl.ds(pl.multiple_of(o * 128, 128), 128)
        hi = jnp.floor((code + 0.5) * (1.0 / (3 * GB)))
        lo = code - 3 * GB * hi
        i = iota((48, 128), 0)
        h = jnp.where(i < 24, i, i - 24).astype(F32)
        hm_ref[:, at] = jnp.where(h == hi, 1.0, 0.0).astype(BF16)
        k = iota((256, 128), 0).astype(F32)
        by_lane = jnp.where(k == lo, 1.0, 0.0).astype(BF16)
        oh_ref[pl.ds(pl.multiple_of(lax.rem(o + 8, TILES) * 128, 128), 128), :] = lax.dot_general(
            identity, by_lane, NT, preferred_element_type=F32
        ).astype(BF16)

    def main_picks(q, carry):
        for j in range(4):
            picks(4 * q + j, codes_ref[4 * q + j, :, :128])
        return carry

    def rem_picks(q, carry):
        quarter = iota((1, 128), 1) // 32
        for j in range(4):
            g = 4 * q + j
            code = codes_ref[4 * g, :, 128:]
            for e in range(1, 4):
                code = jnp.where(quarter == e, codes_ref[4 * g + e, :, 128:], code)
            picks(32 + g, code)
        return carry

    lax.fori_loop(0, NF // 4, main_picks, 0)
    lax.fori_loop(0, 2, rem_picks, 0)

    wait_one(0)
    wait_group(0, 0)
    wait_group(0, 1)

    def shuffle(g, carry):
        tiles = [rec_ref[0, 4 * g + j].astype(F32) for j in range(4)]
        quarter = iota((ROWS, 128), 1) // 32
        for b4 in range(4):
            done = jnp.zeros((ROWS, 128), F32)
            for j in range(4):
                shift = (32 * (j - b4)) % 128
                moved = tiles[j] if shift == 0 else pltpu.roll(tiles[j], shift, 1)
                done = jnp.where(quarter == j, moved, done)
            rec_ref[1 + b4, 32 + g] = done.astype(BF16)
        return carry

    lax.fori_loop(0, 8, shuffle, 0)

    rows = [part * 16 + r for part in range(2) for r in range(PAIRS)]

    def spread(b4, first, lhs_ref):
        for j in range(STEP):
            tile = lax.rem(NF + first + j, TILES)
            values = rec_ref[1 + b4, tile].astype(F32)
            picked = hm_ref[:, pl.ds(pl.multiple_of(tile * 128, 128), 128)]
            lanes = slice(j * 128, j * 128 + 128)
            for i in range(PAIRS):
                a = jnp.broadcast_to(values[rows[2 * i] : rows[2 * i] + 1], (8, 128))
                b = jnp.broadcast_to(values[rows[2 * i + 1] : rows[2 * i + 1] + 1], (8, 128))
                for e, pair in enumerate(((a, a), (a, b), (b, b))):
                    m = 48 * i + 16 * e
                    lhs_ref[m : m + 16, lanes] = (
                        jnp.concatenate(pair, axis=0).astype(BF16)
                        * picked[16 * e : 16 * e + 16]
                    )

    def place(first, lhs_ref):
        at = pl.ds(pl.multiple_of(first * 128, 128), STEP * 128)
        acc_ref[...] += jnp.dot(lhs_ref[...], oh_ref[at, :], preferred_element_type=F32)

    def stage(b4, carry):
        wait_one(1 + b4)
        acc_ref[...] = jnp.zeros_like(acc_ref)

        def half(i, c):
            wait_group(1 + b4, i)
            spread(b4, 20 * i, lhs_a)
            place(20 * i, lhs_a)
            spread(b4, 20 * i + 10, lhs_b)
            place(20 * i + 10, lhs_b)
            return c

        lax.fori_loop(0, 2, half, 0)
        half_rows = PAIRS * HI
        g_ref[:, :256] = acc_ref[:half_rows].astype(BF16)
        g_ref[:, 256:] = acc_ref[half_rows:].astype(BF16)

        for block in range(6):
            at = slice(block * 256, (block + 1) * 256)
            got = jnp.dot(g_ref[...], rt_ref[:, at], preferred_element_type=F32)
            hs_ref[:, block * HI : (block + 1) * HI, :] = got.reshape(PAIRS, HI, 256)
        for p in range(PLANES):
            total = sum_ref[p]
            for bg in range(3):
                wave = jnp.dot(
                    ct_ref[...], hs_ref[bg * PLANES + p].astype(BF16),
                    preferred_element_type=F32,
                )
                re, im = wave[:N], wave[N:]
                total += (re * re + im * im) * (occ_ref[bg * 4 + b4] * (1.0 / (BANDS_HERE * NB)))
            sum_ref[p] = total
        return carry

    loads[2].wait()
    loads[3].wait()
    lax.fori_loop(0, 4, stage, 0)

    folded = iota((16, 128), 1) // 16
    for j in range(NB):
        for p in range(PLANES):
            stage_ref[j, XB * p : XB * (p + 1), :] = sum_ref[p, XB * j : XB * (j + 1), :]
        stage_ref[j, 90:96, :] = jnp.zeros((6, 256), F32)
        extra = jnp.zeros((16, 128), F32)
        for i in range(6):
            piece = stage_ref[j, 16 * i : 16 * i + 16, 128:]
            if i:
                piece = pltpu.roll(piece, 16 * i, 1)
            extra = jnp.where(folded == i, piece, extra)
        bsend_ref[j, :96] = stage_ref[j, :, :128].astype(BF16)
        bsend_ref[j, 96:] = extra.astype(BF16)
    for o in range(1, NB):
        to = lax.rem(band + o, NB)
        pltpu.make_async_remote_copy(
            src_ref=bsend_ref.at[to],
            dst_ref=brec_ref.at[o],
            send_sem=bssem,
            recv_sem=brsem,
            device_id=(me, to),
            device_id_type=MESH,
        ).start()
    band_blocks = pltpu.make_async_remote_copy(
        src_ref=bsend_ref.at[pl.ds(1, NB - 1)],
        dst_ref=brec_ref.at[pl.ds(1, NB - 1)],
        send_sem=bssem,
        recv_sem=brsem,
        device_id=(me, lax.rem(band + 1, NB)),
        device_id_type=MESH,
    )
    total = bsend_ref[band].astype(F32)
    for c in range(CHUNKS):
        blocks(c, 0, NF - 1, 0).wait_send()
    band_blocks.wait_recv()
    for o in range(1, NB):
        total += brec_ref[o].astype(F32)
    tot_ref[:, :128] = total[:96]
    for i in range(6):
        piece = total[96:]
        if i:
            piece = pltpu.roll(piece, 128 - 16 * i, 1)
        tot_ref[16 * i : 16 * i + 16, 128:] = piece
    for p in range(PLANES):
        out_ref[p] = tot_ref[XB * p : XB * (p + 1), :N]
    band_blocks.wait_send()
    every_code.wait_send()


def shards(coefficients, occupations, columns, counts, plane_slot):
    vmem = pl.BlockSpec(memory_space=pltpu.VMEM)
    smem = pl.BlockSpec(memory_space=pltpu.SMEM)
    hbm = pl.BlockSpec(memory_space=pltpu.HBM)
    rows = 2 * PAIRS * HI
    return pl.pallas_call(
        kernel,
        out_shape=jax.ShapeDtypeStruct((PLANES, XB, N), F32),
        in_specs=[hbm, hbm, hbm, hbm, vmem, smem, smem, smem],
        out_specs=vmem,
        scratch_shapes=[
            pltpu.VMEM((BANDS_HERE, SLOTS * 2 * GB), BF16),
            pltpu.VMEM((2 * N, 256), BF16),
            pltpu.VMEM((512, 1536), BF16),
            pltpu.VMEM((2 * N, 6 * HI), BF16),
            pltpu.VMEM((2880, 128), F32),
            pltpu.VMEM((4, 32, 768), F32),
            pltpu.VMEM((NF * ROWS, 2 * N), BF16),
            pltpu.VMEM((NF * ROWS, 768), BF16),
            pltpu.VMEM((CHUNKS, 128, 768), BF16),
            pltpu.VMEM((1, 256), F32),
            pltpu.VMEM((NF, 1, 256), F32),
            pltpu.VMEM((CHUNKS, NF, ROWS, 128), BF16),
            pltpu.VMEM((CHUNKS, TILES, ROWS, 128), BF16),
            pltpu.VMEM((48, KALL), BF16),
            pltpu.VMEM((KALL, 256), BF16),
            pltpu.VMEM((rows, STEP * 128), BF16),
            pltpu.VMEM((rows, STEP * 128), BF16),
            pltpu.VMEM((rows, 256), F32),
            pltpu.VMEM((PAIRS * HI, 512), BF16),
            pltpu.VMEM((PAIRS, 6 * HI, 256), F32),
            pltpu.VMEM((PLANES, N, 256), F32),
            pltpu.VMEM((NB, 96, 256), F32),
            pltpu.VMEM((NB, 112, 128), BF16),
            pltpu.VMEM((NB, 112, 128), BF16),
            pltpu.VMEM((96, 256), F32),
            pltpu.SemaphoreType.DMA((4,)),
            pltpu.SemaphoreType.DMA,
            pltpu.SemaphoreType.DMA,
            pltpu.SemaphoreType.DMA((CHUNKS,)),
            pltpu.SemaphoreType.DMA((CHUNKS, 3)),
            pltpu.SemaphoreType.DMA,
            pltpu.SemaphoreType.DMA,
        ],
        compiler_params=pltpu.CompilerParams(
            collective_id=0, has_side_effects=True, vmem_limit_bytes=60 * 1024 * 1024
        ),
    )(
        coefficients, stick_rows(), row_table(), column_table(),
        columns.reshape(1, SLOTS), plane_slot, counts, occupations,
    )


def solution(mesh):
    placed = (P("band", "fft"), P("band"), P("fft"), P("fft"), P())
    return jax.shard_map(
        shards, mesh=mesh, in_specs=placed, out_specs=P("fft", "band", None), check_vma=False
    )
```

```python
import functools

import jax
import jax.numpy as jnp
import numpy as np
from jax import lax
from jax.experimental import pallas as pl
from jax.experimental.pallas import tpu as pltpu
from jax.sharding import PartitionSpec as P

N = 144
GB = 72
BANDS_HERE = 12
SLOTS = 160
PLANES = 5
NF = 32
NB = 8
Z, Y = 8, 4
PAIRS = 15
ROWS = 32
TILES = 40
KALL = TILES * 128
HI = 24
STEP = 10
CHUNKS = 5
XB = N // NB
F32 = jnp.float32
BF16 = jnp.bfloat16
MESH = pl.DeviceIdType.MESH

NT = (((1,), (1,)), ((), ()))


def trig(freqs, positions):
    turns = np.mod(freqs[:, None] * positions[None, :], N)
    angles = turns * (2.0 * np.pi / N)
    return np.cos(angles), np.sin(angles)


def stick_rows():
    cosine, sine = trig(np.arange(GB) - GB // 2, np.arange(N))
    rows = np.zeros((2 * N, 256), np.float32)
    rows[:N, :GB] = cosine.T
    rows[:N, GB : 2 * GB] = -sine.T
    rows[N:, :GB] = sine.T
    rows[N:, GB : 2 * GB] = cosine.T
    return jnp.asarray(rows, BF16)


def row_table():
    cosine, sine = trig(np.arange(GB) - GB // 2, np.arange(N))
    table = np.zeros((2, 256, 6, 256), np.float32)
    for third in range(3):
        at = slice(third * GB, (third + 1) * GB)
        table[0, at, third * 2, :N] = cosine
        table[0, at, third * 2 + 1, :N] = sine
        table[1, at, third * 2, :N] = -sine
        table[1, at, third * 2 + 1, :N] = cosine
    return jnp.asarray(table.reshape(512, 1536), BF16)


def column_table():
    cosine, sine = trig(np.arange(GB) - GB // 2, np.arange(N))
    table = np.zeros((2, N, 6, HI), np.float32)
    for third in range(3):
        c, s = cosine[third::3].T, sine[third::3].T
        table[0, :, third * 2] = c
        table[0, :, third * 2 + 1] = -s
        table[1, :, third * 2] = s
        table[1, :, third * 2 + 1] = c
    return jnp.asarray(table.reshape(2 * N, 6 * HI), BF16)


ORDER = [0] + [Y * dz + dy for dy in (2, 1, 3, 0) for dz in (1, 7, 2, 6, 3, 5, 4, 0)][:-1]


FAR_FIRST = sorted(
    range(1, NF), key=lambda o: -min(o // Y, Z - o // Y) - min(o % Y, Y - o % Y)
)


def iota(shape, dim):
    return lax.broadcasted_iota(jnp.int32, shape, dim)


def kernel(
    x_hbm, trow_hbm, rt_hbm, ct_hbm, cols_ref, slot_ref, counts_ref, occ_ref,
    out_ref,
    x_ref, trow_ref, rt_ref, ct_ref, xf_ref, xr_ref, chosen_ref, w_ref, xc_ref, code_ref,
    send_ref, rec_ref, hm_ref, oh_ref, lhs_a, lhs_b, acc_ref,
    g_ref, hs_ref, sum_ref, stage_ref, bsend_ref, brec_ref, tot_ref,
    ldsem, ssem, rsem, bssem, brsem,
):
    me = lax.axis_index("fft")
    band = lax.axis_index("band")
    my_z, my_y = me // Y, lax.rem(me, Y)

    def peer(o):
        dz, dy = o // Y, o % Y
        return lax.rem(my_z + dz, Z) * Y + lax.rem(my_y + dy, Y)

    barrier = pltpu.get_barrier_semaphore()
    for o in FAR_FIRST:
        pl.semaphore_signal(barrier, inc=1, device_id=(peer(o), band), device_id_type=MESH)
    for o in range(1, NB):
        pl.semaphore_signal(
            barrier, inc=1, device_id=(me, lax.rem(band + o, NB)), device_id_type=MESH
        )

    loads = [
        pltpu.make_async_copy(src, dst, ldsem.at[i])
        for i, (src, dst) in enumerate(
            ((trow_hbm, trow_ref), (x_hbm, x_ref), (rt_hbm, rt_ref), (ct_hbm, ct_ref))
        )
    ]
    for load in loads:
        load.start()

    def choose(d, carry):
        shape = (ROWS, 2 * N)
        row = iota(shape, 0)
        within = lax.rem(row, 16)
        plane = jnp.where(within < PAIRS, lax.rem(within, PLANES), PLANES)
        index = jnp.full(shape, -1, jnp.int32)
        for p in range(PLANES):
            index = jnp.where(plane == p, slot_ref[d * PLANES + p], index)
        hit = (iota(shape, 1) - N * (row // 16) == index) & (index >= 0)
        chosen_ref[pl.ds(pl.multiple_of(d * ROWS, ROWS), ROWS), :] = jnp.where(
            hit, 1.0, 0.0
        ).astype(BF16)
        return carry

    lax.fori_loop(0, NF, choose, 0)
    loads[0].wait()
    base = jnp.dot(chosen_ref[...], trow_ref[...], preferred_element_type=F32)
    within = lax.rem(iota((NF * ROWS, 256), 0), 16)
    for bg in range(3):
        keep = (within >= bg * PLANES) & (within < bg * PLANES + PLANES)
        w_ref[:, bg * 256 : (bg + 1) * 256] = jnp.where(keep, base, 0.0).astype(BF16)

    shape = (SLOTS, 256)
    l = iota(shape, 1)
    r = lax.rem(l, 32)
    wanted = jnp.where(l < 128, 8 * lax.rem(l, 16) + l // 16, 128 + 8 * lax.rem(r, 4) + r // 4)
    order = jnp.where(iota(shape, 0) == wanted, 1.0, 0.0).astype(BF16)
    col = jnp.broadcast_to(cols_ref[...].astype(F32), (16, SLOTS))
    gx = jnp.floor((col + 0.5) * (1.0 / GB))
    gy = col - gx * GB
    natural = jnp.where(iota((16, SLOTS), 0) == 0, gx, gy).astype(BF16)
    ordered = jnp.dot(natural, order, preferred_element_type=F32)
    code = ordered[0:1] * GB + ordered[1:2]
    high = jnp.floor(code * (1.0 / 64))
    low = code - 64 * high
    coded = (128 + high) * 2.0**-32
    for bit in (32, 16, 8, 4, 2, 1):
        coded = jnp.where(low >= bit, coded * 2.0**bit, coded)
        low = jnp.where(low >= bit, low - bit, low)
    code_ref[...] = coded

    loads[1].wait()

    def widen(g, carry):
        for t in range(9):
            at = pl.ds(pl.multiple_of(g * 1152 + t * 128, 128), 128)
            xf_ref[pl.ds(pl.multiple_of((g * 9 + t) * 16, 16), BANDS_HERE), :] = x_ref[
                :, at
            ].astype(F32)
        return carry

    lax.fori_loop(0, 20, widen, 0)
    lane20 = iota((20, 128), 1)
    for b in range(BANDS_HERE):
        bg, b4 = b // 4, b % 4
        tiles = [xf_ref[pl.ds(t * 16 + b, 20, 144), :] for t in range(9)]
        for t in range(8):
            if t == 0:
                first, second = tiles[0], tiles[1]
            else:
                second = pltpu.roll(tiles[t + 1], 128 - 16 * t, 1)
                first = jnp.where(
                    lane20 < 128 - 16 * t, pltpu.roll(tiles[t], 128 - 16 * t, 1), second
                )
            for e, value in enumerate((first, second)):
                lanes = slice(bg * 256 + e * 128, bg * 256 + e * 128 + 128)
                xc_ref[1 + b4, 16 * t : 16 * t + 16, lanes] = value[:16].astype(BF16)
                xr_ref[b4, 4 * t : 4 * t + 4, lanes] = value[16:20]
    for b4 in range(4):
        xc_ref[0, 32 * b4 : 32 * b4 + 32, :] = xr_ref[b4].astype(BF16)

    lane = iota((1, 128), 1)
    count = counts_ref[0]
    row32 = iota((ROWS, 128), 0)

    def outgoing(c):
        r = lax.rem(lane, 32)
        slot = jnp.where(
            c == 0, 128 + 8 * lax.rem(r, 4) + r // 4, 8 * lax.rem(lane, 16) + lane // 16
        )
        live = jnp.where(slot < count, 1.0, 0.0)
        res = lax.dot_general(w_ref[...], xc_ref[c], NT, preferred_element_type=F32) * live
        codes = code_ref[...]
        aux = jnp.where(row32 == 15, codes[:, :128], jnp.where(row32 == 31, codes[:, 128:], 0.0))
        send_ref[c] = (res.reshape(NF, ROWS, 128) + aux[None]).astype(BF16)

    def block_copy(c, i):
        return pltpu.make_async_remote_copy(
            src_ref=send_ref.at[c, peer(ORDER[i])],
            dst_ref=rec_ref.at[c, i],
            send_sem=ssem.at[c],
            recv_sem=rsem.at[c, i // 16 if i != 16 else 2],
            device_id=(peer(ORDER[i]), band),
            device_id_type=MESH,
        )

    def blocks(c, first, size, group):
        return pltpu.make_async_remote_copy(
            src_ref=send_ref.at[c, pl.ds(0, size)],
            dst_ref=rec_ref.at[c, pl.ds(first, size)],
            send_sem=ssem.at[c],
            recv_sem=rsem.at[c, group],
            device_id=(peer(1), band),
            device_id_type=MESH,
        )

    def wait_one(c):
        blocks(c, 16, 1, 2).wait_recv()

    def wait_group(c, group):
        blocks(c, 1 + 16 * group, 15, group).wait_recv()

    outgoing(0)
    pl.semaphore_wait(barrier, NF - 1 + NB - 1)

    def send_chunk(c, carry):
        @pl.when(c > 0)
        def _():
            outgoing(c)

        for i in range(1, NF):
            block_copy(c, i).start()
        rec_ref[c, 0] = send_ref[c, me]
        return carry

    lax.fori_loop(0, CHUNKS, send_chunk, 0)

    sum_ref[...] = jnp.zeros_like(sum_ref)

    wait_one(0)
    wait_group(0, 0)
    wait_group(0, 1)
    identity = jnp.where(iota((128, 128), 0) == iota((128, 128), 1), 1.0, 0.0).astype(BF16)

    def picks(o, coded):
        high, code = coded * 2.0**32, jnp.zeros((1, 128), F32)
        for bit in (32, 16, 8, 4, 2, 1):
            above = high >= 128 * 2.0**bit
            high = jnp.where(above, high * 2.0**-bit, high)
            code = jnp.where(above, code + bit, code)
        code += (high - 128) * 64
        at = pl.ds(pl.multiple_of(o * 128, 128), 128)
        hi = jnp.floor((code + 0.5) * (1.0 / (3 * GB)))
        lo = code - 3 * GB * hi
        i = iota((48, 128), 0)
        h = jnp.where(i < 24, i, i - 24).astype(F32)
        hm_ref[:, at] = jnp.where(h == hi, 1.0, 0.0).astype(BF16)
        k = iota((256, 128), 0).astype(F32)
        by_lane = jnp.where(k == lo, 1.0, 0.0).astype(BF16)
        oh_ref[pl.ds(pl.multiple_of(lax.rem(o + 8, TILES) * 128, 128), 128), :] = lax.dot_general(
            identity, by_lane, NT, preferred_element_type=F32
        ).astype(BF16)

    def main_picks(q, carry):
        for j in range(4):
            picks(4 * q + j, rec_ref[0, 4 * q + j].astype(F32)[15:16])
        return carry

    def rem_picks(q, carry):
        quarter = iota((1, 128), 1) // 32
        for j in range(4):
            g = 4 * q + j
            code = rec_ref[0, 4 * g].astype(F32)[31:32]
            for e in range(1, 4):
                code = jnp.where(quarter == e, rec_ref[0, 4 * g + e].astype(F32)[31:32], code)
            picks(32 + g, code)
        return carry

    lax.fori_loop(0, NF // 4, main_picks, 0)
    lax.fori_loop(0, 2, rem_picks, 0)


    def shuffle(g, carry):
        tiles = [rec_ref[0, 4 * g + j].astype(F32) for j in range(4)]
        quarter = iota((ROWS, 128), 1) // 32
        for b4 in range(4):
            done = jnp.zeros((ROWS, 128), F32)
            for j in range(4):
                shift = (32 * (j - b4)) % 128
                moved = tiles[j] if shift == 0 else pltpu.roll(tiles[j], shift, 1)
                done = jnp.where(quarter == j, moved, done)
            rec_ref[1 + b4, 32 + g] = done.astype(BF16)
        return carry

    lax.fori_loop(0, 8, shuffle, 0)

    rows = [part * 16 + r for part in range(2) for r in range(PAIRS)]

    def spread(b4, first, lhs_ref):
        for j in range(STEP):
            tile = lax.rem(NF + first + j, TILES)
            values = rec_ref[1 + b4, tile].astype(F32)
            picked = hm_ref[:, pl.ds(pl.multiple_of(tile * 128, 128), 128)]
            lanes = slice(j * 128, j * 128 + 128)
            for i in range(PAIRS):
                a = jnp.broadcast_to(values[rows[2 * i] : rows[2 * i] + 1], (8, 128))
                b = jnp.broadcast_to(values[rows[2 * i + 1] : rows[2 * i + 1] + 1], (8, 128))
                for e, pair in enumerate(((a, a), (a, b), (b, b))):
                    m = 48 * i + 16 * e
                    lhs_ref[m : m + 16, lanes] = (
                        jnp.concatenate(pair, axis=0).astype(BF16)
                        * picked[16 * e : 16 * e + 16]
                    )

    def place(first, lhs_ref):
        at = pl.ds(pl.multiple_of(first * 128, 128), STEP * 128)
        acc_ref[...] += jnp.dot(lhs_ref[...], oh_ref[at, :], preferred_element_type=F32)

    def stage(b4, carry):
        wait_one(1 + b4)
        acc_ref[...] = jnp.zeros_like(acc_ref)

        def half(i, c):
            wait_group(1 + b4, i)
            spread(b4, 20 * i, lhs_a)
            place(20 * i, lhs_a)
            spread(b4, 20 * i + 10, lhs_b)
            place(20 * i + 10, lhs_b)
            return c

        lax.fori_loop(0, 2, half, 0)
        half_rows = PAIRS * HI
        g_ref[:, :256] = acc_ref[:half_rows].astype(BF16)
        g_ref[:, 256:] = acc_ref[half_rows:].astype(BF16)

        for block in range(6):
            at = slice(block * 256, (block + 1) * 256)
            got = jnp.dot(g_ref[...], rt_ref[:, at], preferred_element_type=F32)
            hs_ref[:, block * HI : (block + 1) * HI, :] = got.reshape(PAIRS, HI, 256)
        for p in range(PLANES):
            total = sum_ref[p]
            for bg in range(3):
                wave = jnp.dot(
                    ct_ref[...], hs_ref[bg * PLANES + p].astype(BF16),
                    preferred_element_type=F32,
                )
                re, im = wave[:N], wave[N:]
                total += (re * re + im * im) * (occ_ref[bg * 4 + b4] * (1.0 / (BANDS_HERE * NB)))
            sum_ref[p] = total
        return carry

    loads[2].wait()
    loads[3].wait()
    lax.fori_loop(0, 4, stage, 0)

    folded = iota((16, 128), 1) // 16
    for j in range(NB):
        for p in range(PLANES):
            stage_ref[j, XB * p : XB * (p + 1), :] = sum_ref[p, XB * j : XB * (j + 1), :]
        stage_ref[j, 90:96, :] = jnp.zeros((6, 256), F32)
        extra = jnp.zeros((16, 128), F32)
        for i in range(6):
            piece = stage_ref[j, 16 * i : 16 * i + 16, 128:]
            if i:
                piece = pltpu.roll(piece, 16 * i, 1)
            extra = jnp.where(folded == i, piece, extra)
        bsend_ref[j, :96] = stage_ref[j, :, :128].astype(BF16)
        bsend_ref[j, 96:] = extra.astype(BF16)
    for o in range(1, NB):
        to = lax.rem(band + o, NB)
        pltpu.make_async_remote_copy(
            src_ref=bsend_ref.at[to],
            dst_ref=brec_ref.at[o],
            send_sem=bssem,
            recv_sem=brsem,
            device_id=(me, to),
            device_id_type=MESH,
        ).start()
    band_blocks = pltpu.make_async_remote_copy(
        src_ref=bsend_ref.at[pl.ds(1, NB - 1)],
        dst_ref=brec_ref.at[pl.ds(1, NB - 1)],
        send_sem=bssem,
        recv_sem=brsem,
        device_id=(me, lax.rem(band + 1, NB)),
        device_id_type=MESH,
    )
    total = bsend_ref[band].astype(F32)
    for c in range(CHUNKS):
        blocks(c, 0, NF - 1, 0).wait_send()
    band_blocks.wait_recv()
    for o in range(1, NB):
        total += brec_ref[o].astype(F32)
    tot_ref[:, :128] = total[:96]
    for i in range(6):
        piece = total[96:]
        if i:
            piece = pltpu.roll(piece, 128 - 16 * i, 1)
        tot_ref[16 * i : 16 * i + 16, 128:] = piece
    for p in range(PLANES):
        out_ref[p] = tot_ref[XB * p : XB * (p + 1), :N]
    band_blocks.wait_send()


def shards(coefficients, occupations, columns, counts, plane_slot):
    vmem = pl.BlockSpec(memory_space=pltpu.VMEM)
    smem = pl.BlockSpec(memory_space=pltpu.SMEM)
    hbm = pl.BlockSpec(memory_space=pltpu.HBM)
    rows = 2 * PAIRS * HI
    return pl.pallas_call(
        kernel,
        out_shape=jax.ShapeDtypeStruct((PLANES, XB, N), F32),
        in_specs=[hbm, hbm, hbm, hbm, vmem, smem, smem, smem],
        out_specs=vmem,
        scratch_shapes=[
            pltpu.VMEM((BANDS_HERE, SLOTS * 2 * GB), BF16),
            pltpu.VMEM((2 * N, 256), BF16),
            pltpu.VMEM((512, 1536), BF16),
            pltpu.VMEM((2 * N, 6 * HI), BF16),
            pltpu.VMEM((2880, 128), F32),
            pltpu.VMEM((4, 32, 768), F32),
            pltpu.VMEM((NF * ROWS, 2 * N), BF16),
            pltpu.VMEM((NF * ROWS, 768), BF16),
            pltpu.VMEM((CHUNKS, 128, 768), BF16),
            pltpu.VMEM((1, 256), F32),
            pltpu.VMEM((CHUNKS, NF, ROWS, 128), BF16),
            pltpu.VMEM((CHUNKS, TILES, ROWS, 128), BF16),
            pltpu.VMEM((48, KALL), BF16),
            pltpu.VMEM((KALL, 256), BF16),
            pltpu.VMEM((rows, STEP * 128), BF16),
            pltpu.VMEM((rows, STEP * 128), BF16),
            pltpu.VMEM((rows, 256), F32),
            pltpu.VMEM((PAIRS * HI, 512), BF16),
            pltpu.VMEM((PAIRS, 6 * HI, 256), F32),
            pltpu.VMEM((PLANES, N, 256), F32),
            pltpu.VMEM((NB, 96, 256), F32),
            pltpu.VMEM((NB, 112, 128), BF16),
            pltpu.VMEM((NB, 112, 128), BF16),
            pltpu.VMEM((96, 256), F32),
            pltpu.SemaphoreType.DMA((4,)),
            pltpu.SemaphoreType.DMA((CHUNKS,)),
            pltpu.SemaphoreType.DMA((CHUNKS, 3)),
            pltpu.SemaphoreType.DMA,
            pltpu.SemaphoreType.DMA,
        ],
        compiler_params=pltpu.CompilerParams(
            collective_id=0, has_side_effects=True, vmem_limit_bytes=60 * 1024 * 1024
        ),
    )(
        coefficients, stick_rows(), row_table(), column_table(),
        columns.reshape(1, SLOTS), plane_slot, counts, occupations,
    )


def solution(mesh):
    placed = (P("band", "fft"), P("band"), P("fft"), P("fft"), P())
    return jax.shard_map(
        shards, mesh=mesh, in_specs=placed, out_specs=P("fft", "band", None), check_vma=False
    )
```

```python
import functools

import jax
import jax.numpy as jnp
import numpy as np
from jax import lax
from jax.experimental import pallas as pl
from jax.experimental.pallas import tpu as pltpu
from jax.sharding import PartitionSpec as P

N = 144
GB = 72
BANDS_HERE = 12
SLOTS = 160
PLANES = 5
NF = 32
NB = 8
Z, Y = 8, 4
PAIRS = 15
ROWS = 32
TILES = 40
KALL = TILES * 128
HI = 24
STEP = 10
CHUNKS = 5
XB = N // NB
F32 = jnp.float32
BF16 = jnp.bfloat16
MESH = pl.DeviceIdType.MESH

NT = (((1,), (1,)), ((), ()))


def trig(freqs, positions):
    turns = np.mod(freqs[:, None] * positions[None, :], N)
    angles = turns * (2.0 * np.pi / N)
    return np.cos(angles), np.sin(angles)


def stick_rows():
    cosine, sine = trig(np.arange(GB) - GB // 2, np.arange(N))
    rows = np.zeros((2 * N, 256), np.float32)
    rows[:N, :GB] = cosine.T
    rows[:N, GB : 2 * GB] = -sine.T
    rows[N:, :GB] = sine.T
    rows[N:, GB : 2 * GB] = cosine.T
    return jnp.asarray(rows, BF16)


def row_table():
    cosine, sine = trig(np.arange(GB) - GB // 2, np.arange(N))
    table = np.zeros((2, 256, 6, 256), np.float32)
    for third in range(3):
        at = slice(third * GB, (third + 1) * GB)
        table[0, at, third * 2, :N] = cosine
        table[0, at, third * 2 + 1, :N] = sine
        table[1, at, third * 2, :N] = -sine
        table[1, at, third * 2 + 1, :N] = cosine
    return jnp.asarray(table.reshape(512, 1536), BF16)


def column_table():
    cosine, sine = trig(np.arange(GB) - GB // 2, np.arange(N))
    table = np.zeros((2, N, 6, HI), np.float32)
    for third in range(3):
        c, s = cosine[third::3].T, sine[third::3].T
        table[0, :, third * 2] = c
        table[0, :, third * 2 + 1] = -s
        table[1, :, third * 2] = s
        table[1, :, third * 2 + 1] = c
    return jnp.asarray(table.reshape(2 * N, 6 * HI), BF16)


ORDER = [0] + [Y * dz + dy for dy in (2, 1, 3, 0) for dz in (1, 7, 2, 6, 3, 5, 4, 0)][:-1]


FAR_FIRST = sorted(
    range(1, NF), key=lambda o: -min(o // Y, Z - o // Y) - min(o % Y, Y - o % Y)
)


def iota(shape, dim):
    return lax.broadcasted_iota(jnp.int32, shape, dim)


def kernel(
    x_hbm, trow_hbm, rt_hbm, ct_hbm, cols_ref, slot_ref, counts_ref, occ_ref,
    out_ref,
    x_ref, trow_ref, rt_ref, ct_ref, xf_ref, xr_ref, chosen_ref, w_ref, xc_ref, code_ref,
    send_ref, rec_ref, hm_ref, oh_ref, lhs_a, lhs_b, acc_ref,
    g_ref, hs_ref, sum_ref, stage_ref, bsend_ref, brec_ref, tot_ref,
    ldsem, ssem, rsem, bssem, brsem,
):
    me = lax.axis_index("fft")
    band = lax.axis_index("band")
    my_z, my_y = me // Y, lax.rem(me, Y)

    def peer(o):
        dz, dy = o // Y, o % Y
        return lax.rem(my_z + dz, Z) * Y + lax.rem(my_y + dy, Y)

    barrier = pltpu.get_barrier_semaphore()
    for o in FAR_FIRST:
        pl.semaphore_signal(barrier, inc=1, device_id=(peer(o), band), device_id_type=MESH)
    for o in range(1, NB):
        pl.semaphore_signal(
            barrier, inc=1, device_id=(me, lax.rem(band + o, NB)), device_id_type=MESH
        )

    loads = [
        pltpu.make_async_copy(src, dst, ldsem.at[i])
        for i, (src, dst) in enumerate(
            ((trow_hbm, trow_ref), (x_hbm, x_ref), (rt_hbm, rt_ref), (ct_hbm, ct_ref))
        )
    ]
    for load in loads:
        load.start()

    def choose(d, carry):
        shape = (ROWS, 2 * N)
        row = iota(shape, 0)
        within = lax.rem(row, 16)
        plane = jnp.where(within < PAIRS, lax.rem(within, PLANES), PLANES)
        index = jnp.full(shape, -1, jnp.int32)
        for p in range(PLANES):
            index = jnp.where(plane == p, slot_ref[d * PLANES + p], index)
        hit = (iota(shape, 1) - N * (row // 16) == index) & (index >= 0)
        chosen_ref[pl.ds(pl.multiple_of(d * ROWS, ROWS), ROWS), :] = jnp.where(
            hit, 1.0, 0.0
        ).astype(BF16)
        return carry

    lax.fori_loop(0, NF, choose, 0)
    loads[0].wait()
    base = jnp.dot(chosen_ref[...], trow_ref[...], preferred_element_type=F32)
    within = lax.rem(iota((NF * ROWS, 256), 0), 16)
    for bg in range(3):
        keep = (within >= bg * PLANES) & (within < bg * PLANES + PLANES)
        w_ref[:, bg * 256 : (bg + 1) * 256] = jnp.where(keep, base, 0.0).astype(BF16)

    shape = (SLOTS, 256)
    l = iota(shape, 1)
    r = lax.rem(l, 32)
    wanted = jnp.where(l < 128, 8 * lax.rem(l, 16) + l // 16, 128 + 8 * lax.rem(r, 4) + r // 4)
    order = jnp.where(iota(shape, 0) == wanted, 1.0, 0.0).astype(BF16)
    col = jnp.broadcast_to(cols_ref[...].astype(F32), (16, SLOTS))
    gx = jnp.floor((col + 0.5) * (1.0 / GB))
    gy = col - gx * GB
    natural = jnp.where(iota((16, SLOTS), 0) == 0, gx, gy).astype(BF16)
    ordered = jnp.dot(natural, order, preferred_element_type=F32)
    code = ordered[0:1] * GB + ordered[1:2]
    high = jnp.floor(code * (1.0 / 64))
    low = code - 64 * high
    coded = (128 + high) * 2.0**-32
    for bit in (32, 16, 8, 4, 2, 1):
        coded = jnp.where(low >= bit, coded * 2.0**bit, coded)
        low = jnp.where(low >= bit, low - bit, low)
    code_ref[...] = coded

    loads[1].wait()

    def widen(g, carry):
        for t in range(9):
            at = pl.ds(pl.multiple_of(g * 1152 + t * 128, 128), 128)
            xf_ref[pl.ds(pl.multiple_of((g * 9 + t) * 16, 16), BANDS_HERE), :] = x_ref[
                :, at
            ].astype(F32)
        return carry

    lax.fori_loop(0, 20, widen, 0)
    lane20 = iota((20, 128), 1)
    for b in range(BANDS_HERE):
        bg, b4 = b // 4, b % 4
        tiles = [xf_ref[pl.ds(t * 16 + b, 20, 144), :] for t in range(9)]
        for t in range(8):
            if t == 0:
                first, second = tiles[0], tiles[1]
            else:
                second = pltpu.roll(tiles[t + 1], 128 - 16 * t, 1)
                first = jnp.where(
                    lane20 < 128 - 16 * t, pltpu.roll(tiles[t], 128 - 16 * t, 1), second
                )
            for e, value in enumerate((first, second)):
                lanes = slice(bg * 256 + e * 128, bg * 256 + e * 128 + 128)
                xc_ref[1 + b4, 16 * t : 16 * t + 16, lanes] = value[:16].astype(BF16)
                xr_ref[b4, 4 * t : 4 * t + 4, lanes] = value[16:20]
    for b4 in range(4):
        xc_ref[0, 32 * b4 : 32 * b4 + 32, :] = xr_ref[b4, :32].astype(BF16)

    lane = iota((1, 128), 1)
    count = counts_ref[0]
    row32 = iota((ROWS, 128), 0)

    def outgoing(c):
        r = lax.rem(lane, 32)
        slot = jnp.where(
            c == 0, 128 + 8 * lax.rem(r, 4) + r // 4, 8 * lax.rem(lane, 16) + lane // 16
        )
        live = jnp.where(slot < count, 1.0, 0.0)
        res = lax.dot_general(w_ref[...], xc_ref[c], NT, preferred_element_type=F32) * live
        codes = code_ref[...]
        aux = jnp.where(row32 == 15, codes[:, :128], jnp.where(row32 == 31, codes[:, 128:], 0.0))
        send_ref[c] = (res.reshape(NF, ROWS, 128) + aux[None]).astype(BF16)

    def block_copy(c, i):
        return pltpu.make_async_remote_copy(
            src_ref=send_ref.at[c, peer(ORDER[i])],
            dst_ref=rec_ref.at[c, i],
            send_sem=ssem.at[c],
            recv_sem=rsem.at[c, i // 16 if i != 16 else 2],
            device_id=(peer(ORDER[i]), band),
            device_id_type=MESH,
        )

    def blocks(c, first, size, group):
        return pltpu.make_async_remote_copy(
            src_ref=send_ref.at[c, pl.ds(0, size)],
            dst_ref=rec_ref.at[c, pl.ds(first, size)],
            send_sem=ssem.at[c],
            recv_sem=rsem.at[c, group],
            device_id=(peer(1), band),
            device_id_type=MESH,
        )

    def wait_one(c):
        blocks(c, 16, 1, 2).wait_recv()

    def wait_group(c, group):
        blocks(c, 1 + 16 * group, 15, group).wait_recv()

    outgoing(0)
    pl.semaphore_wait(barrier, NF - 1 + NB - 1)

    def send_chunk(c, carry):
        @pl.when(c > 0)
        def _():
            outgoing(c)

        for i in range(1, NF):
            block_copy(c, i).start()
        rec_ref[c, 0] = send_ref[c, me]
        return carry

    lax.fori_loop(0, CHUNKS, send_chunk, 0)

    sum_ref[...] = jnp.zeros_like(sum_ref)

    wait_one(0)
    wait_group(0, 0)
    wait_group(0, 1)
    identity = jnp.where(iota((128, 128), 0) == iota((128, 128), 1), 1.0, 0.0).astype(BF16)

    def picks(o, coded):
        high, code = coded * 2.0**32, jnp.zeros((1, 128), F32)
        for bit in (32, 16, 8, 4, 2, 1):
            above = high >= 128 * 2.0**bit
            high = jnp.where(above, high * 2.0**-bit, high)
            code = jnp.where(above, code + bit, code)
        code += (high - 128) * 64
        at = pl.ds(pl.multiple_of(o * 128, 128), 128)
        hi = jnp.floor((code + 0.5) * (1.0 / (3 * GB)))
        lo = code - 3 * GB * hi
        i = iota((48, 128), 0)
        h = jnp.where(i < 24, i, i - 24).astype(F32)
        hm_ref[:, at] = jnp.where(h == hi, 1.0, 0.0).astype(BF16)
        k = iota((256, 128), 0).astype(F32)
        by_lane = jnp.where(k == lo, 1.0, 0.0).astype(BF16)
        oh_ref[pl.ds(pl.multiple_of(lax.rem(o + 8, TILES) * 128, 128), 128), :] = lax.dot_general(
            identity, by_lane, NT, preferred_element_type=F32
        ).astype(BF16)

    def main_picks(q, carry):
        for j in range(4):
            picks(4 * q + j, rec_ref[0, 4 * q + j].astype(F32)[15:16])
        return carry

    def rem_picks(q, carry):
        quarter = iota((1, 128), 1) // 32
        for j in range(4):
            g = 4 * q + j
            code = rec_ref[0, 4 * g].astype(F32)[31:32]
            for e in range(1, 4):
                code = jnp.where(quarter == e, rec_ref[0, 4 * g + e].astype(F32)[31:32], code)
            picks(32 + g, code)
        return carry

    lax.fori_loop(0, NF // 4, main_picks, 0)
    lax.fori_loop(0, 2, rem_picks, 0)


    def shuffle(g, carry):
        tiles = [rec_ref[0, 4 * g + j].astype(F32) for j in range(4)]
        quarter = iota((ROWS, 128), 1) // 32
        for b4 in range(4):
            done = jnp.zeros((ROWS, 128), F32)
            for j in range(4):
                shift = (32 * (j - b4)) % 128
                moved = tiles[j] if shift == 0 else pltpu.roll(tiles[j], shift, 1)
                done = jnp.where(quarter == j, moved, done)
            rec_ref[1 + b4, 32 + g] = done.astype(BF16)
        return carry

    lax.fori_loop(0, 8, shuffle, 0)

    rows = [part * 16 + r for part in range(2) for r in range(PAIRS)]

    def spread(b4, first, lhs_ref):
        for j in range(STEP):
            tile = lax.rem(NF + first + j, TILES)
            values = rec_ref[1 + b4, tile].astype(F32)
            picked = hm_ref[:, pl.ds(pl.multiple_of(tile * 128, 128), 128)]
            lanes = slice(j * 128, j * 128 + 128)
            for i in range(PAIRS):
                a = jnp.broadcast_to(values[rows[2 * i] : rows[2 * i] + 1], (8, 128))
                b = jnp.broadcast_to(values[rows[2 * i + 1] : rows[2 * i + 1] + 1], (8, 128))
                for e, pair in enumerate(((a, a), (a, b), (b, b))):
                    m = 48 * i + 16 * e
                    lhs_ref[m : m + 16, lanes] = (
                        jnp.concatenate(pair, axis=0).astype(BF16)
                        * picked[16 * e : 16 * e + 16]
                    )

    def place(first, lhs_ref):
        at = pl.ds(pl.multiple_of(first * 128, 128), STEP * 128)
        acc_ref[...] += jnp.dot(lhs_ref[...], oh_ref[at, :], preferred_element_type=F32)

    def stage(b4, carry):
        wait_one(1 + b4)
        acc_ref[...] = jnp.zeros_like(acc_ref)

        def half(i, c):
            wait_group(1 + b4, i)
            spread(b4, 20 * i, lhs_a)
            place(20 * i, lhs_a)
            spread(b4, 20 * i + 10, lhs_b)
            place(20 * i + 10, lhs_b)
            return c

        lax.fori_loop(0, 2, half, 0)
        half_rows = PAIRS * HI
        g_ref[:, :256] = acc_ref[:half_rows].astype(BF16)
        g_ref[:, 256:] = acc_ref[half_rows:].astype(BF16)

        for block in range(6):
            at = slice(block * 256, (block + 1) * 256)
            got = jnp.dot(g_ref[...], rt_ref[:, at], preferred_element_type=F32)
            hs_ref[:, block * HI : (block + 1) * HI, :] = got.reshape(PAIRS, HI, 256)
        for p in range(PLANES):
            total = sum_ref[p, :N]
            for bg in range(3):
                wave = jnp.dot(
                    ct_ref[...], hs_ref[bg * PLANES + p].astype(BF16),
                    preferred_element_type=F32,
                )
                re, im = wave[:N], wave[N:]
                total += (re * re + im * im) * (occ_ref[bg * 4 + b4] * (1.0 / (BANDS_HERE * NB)))
            sum_ref[p, :N] = total
        return carry

    loads[2].wait()
    loads[3].wait()
    lax.fori_loop(0, 4, stage, 0)

    folded = iota((16, 128), 1) // 16
    for j in range(NB):
        for p in range(PLANES):
            stage_ref[j, XB * p : XB * (p + 1), :] = sum_ref[p, XB * j : XB * (j + 1), :]
        stage_ref[j, 90:96, :] = jnp.zeros((6, 256), F32)
        extra = jnp.zeros((16, 128), F32)
        for i in range(6):
            piece = stage_ref[j, 16 * i : 16 * i + 16, 128:]
            if i:
                piece = pltpu.roll(piece, 16 * i, 1)
            extra = jnp.where(folded == i, piece, extra)
        bsend_ref[j, :96] = stage_ref[j, :96, :128].astype(BF16)
        bsend_ref[j, 96:] = extra.astype(BF16)
    for o in range(1, NB):
        to = lax.rem(band + o, NB)
        pltpu.make_async_remote_copy(
            src_ref=bsend_ref.at[to],
            dst_ref=brec_ref.at[o],
            send_sem=bssem,
            recv_sem=brsem,
            device_id=(me, to),
            device_id_type=MESH,
        ).start()
    band_blocks = pltpu.make_async_remote_copy(
        src_ref=bsend_ref.at[pl.ds(1, NB - 1)],
        dst_ref=brec_ref.at[pl.ds(1, NB - 1)],
        send_sem=bssem,
        recv_sem=brsem,
        device_id=(me, lax.rem(band + 1, NB)),
        device_id_type=MESH,
    )
    total = bsend_ref[band].astype(F32)
    for c in range(CHUNKS):
        blocks(c, 0, NF - 1, 0).wait_send()
    band_blocks.wait_recv()
    for o in range(1, NB):
        total += brec_ref[o].astype(F32)
    tot_ref[:, :128] = total[:96]
    for i in range(6):
        piece = total[96:]
        if i:
            piece = pltpu.roll(piece, 128 - 16 * i, 1)
        tot_ref[16 * i : 16 * i + 16, 128:] = piece
    for p in range(PLANES):
        out_ref[p] = tot_ref[XB * p : XB * (p + 1), :N]
    band_blocks.wait_send()


def shards(coefficients, occupations, columns, counts, plane_slot):
    vmem = pl.BlockSpec(memory_space=pltpu.VMEM)
    smem = pl.BlockSpec(memory_space=pltpu.SMEM)
    hbm = pl.BlockSpec(memory_space=pltpu.HBM)
    rows = 2 * PAIRS * HI
    return pl.pallas_call(
        kernel,
        out_shape=jax.ShapeDtypeStruct((PLANES, XB, N), F32),
        in_specs=[hbm, hbm, hbm, hbm, vmem, smem, smem, smem],
        out_specs=vmem,
        scratch_shapes=[
            pltpu.VMEM((BANDS_HERE, SLOTS * 2 * GB), BF16),
            pltpu.VMEM((2 * N, 256), BF16),
            pltpu.VMEM((512, 1536), BF16),
            pltpu.VMEM((2 * N, 6 * HI), BF16),
            pltpu.VMEM((3456, 128), F32),
            pltpu.VMEM((4, 40, 768), F32),
            pltpu.VMEM((NF * ROWS, 2 * N), BF16),
            pltpu.VMEM((NF * ROWS, 768), BF16),
            pltpu.VMEM((CHUNKS, 128, 768), BF16),
            pltpu.VMEM((1, 256), F32),
            pltpu.VMEM((CHUNKS, NF, ROWS, 128), BF16),
            pltpu.VMEM((CHUNKS, TILES, ROWS, 128), BF16),
            pltpu.VMEM((48, KALL), BF16),
            pltpu.VMEM((KALL, 256), BF16),
            pltpu.VMEM((rows, STEP * 128), BF16),
            pltpu.VMEM((rows, STEP * 128), BF16),
            pltpu.VMEM((rows, 256), F32),
            pltpu.VMEM((PAIRS * HI, 512), BF16),
            pltpu.VMEM((PAIRS, 6 * HI, 256), F32),
            pltpu.VMEM((PLANES, N + 8, 256), F32),
            pltpu.VMEM((NB, 104, 256), F32),
            pltpu.VMEM((NB, 112, 128), BF16),
            pltpu.VMEM((NB, 112, 128), BF16),
            pltpu.VMEM((96, 256), F32),
            pltpu.SemaphoreType.DMA((4,)),
            pltpu.SemaphoreType.DMA((CHUNKS,)),
            pltpu.SemaphoreType.DMA((CHUNKS, 3)),
            pltpu.SemaphoreType.DMA,
            pltpu.SemaphoreType.DMA,
        ],
        compiler_params=pltpu.CompilerParams(
            collective_id=0, has_side_effects=True, vmem_limit_bytes=60 * 1024 * 1024
        ),
    )(
        coefficients, stick_rows(), row_table(), column_table(),
        columns.reshape(1, SLOTS), plane_slot, counts, occupations,
    )


def solution(mesh):
    placed = (P("band", "fft"), P("band"), P("fft"), P("fft"), P())
    return jax.shard_map(
        shards, mesh=mesh, in_specs=placed, out_specs=P("fft", "band", None), check_vma=False
    )
```
